256 devices in a mesh: chan: 4 (over x), sym: 4 (over z_hi), sub: 16 (over y, z_lo, core).
Axes of the slice: x: 4, y: 4, z: 8 (z_hi: 4, z_lo: 2; z = z_hi * 2 + z_lo), core: 2. Of those that a mesh axis runs over, the one named last changes fastest.
Arguments:
- samples: float32 [2, 64, 24, 9216], P(None, ('chan', 'sub'), 'sym'), parts along dimension 1, may hold values from -16 to 16
- constellation_index: int32 [96, 4096], P(('chan', 'sym'), 'sub'), parts along dimension 0, may hold values from 0 to 63, as said below
- pilot_offsets: int32 [24], P('sym'), may hold values from 0 to 11
- cp_offset: int32 [96], P(('chan', 'sym')), parts along dimension 0, may hold values from 0 to 1024, as said below
Outputs:
- caf: float32 [2, 64, 24, 1024], P(None, 'chan', 'sym', 'sub'), parts along dimension 1
The draws below stay inside these ranges and needn't reach their ends.
There are 4 independent parts, one for each index of `chan`. The reference program is written for one: setup_inputs(seed, part) draws one part's arguments, and reference() takes and returns one part's arrays. A program takes and returns all parts, laid end to end along the dimension named above; an argument that names none is the same for every part. Nothing has to cross between parts.
Inputs may be any that keep to these rules, and one draw needn't show every extreme that they name: Symbol m's scattered pilots sit on the active subcarriers k with k mod 12 == pilot_offsets[m]. The transform window of symbol m is samples cp_offset[m] to cp_offset[m] + 64 * 128 - 1 of its record. `constellation_index`: the index's low three bits give the in-phase level, the high three the quadrature level.
All inputs are finite; a program needn't handle non-finite values.
Results may differ from the reference program's by a relative error of at most 0.0003.
Values may be sent and summed in bfloat16 or wider, within the bound.
A program may use at most 64 MiB of HBM per device.

```python
import math
import jax
import jax.numpy as jnp
from jax import lax

OUTER_FACTOR = 64
INNER_FACTOR = 128
ACTIVE_TONES = 4096
GUARD_SAMPLES = 1024
SMOOTH_HALFSPAN = 48
PSP = 12
CH = 16
SYMBOL_COUNT = 24


TWO_PI = 2.0 * math.pi


HIGHEST = lax.Precision.HIGHEST


def decoded_levels(key):
    return jax.random.randint(jax.random.fold_in(key, 101), (SYMBOL_COUNT, ACTIVE_TONES), 0, 64, dtype=jnp.int32)


def window_starts(key):
    return jax.random.randint(jax.random.fold_in(key, 202), (SYMBOL_COUNT,), 0, GUARD_SAMPLES + 1, dtype=jnp.int32)


def draw_constellation_index(key, part):
    return decoded_levels(key)


def draw_cp_offset(key, part):
    return window_starts(key)


def phase_table(product, period):
    angle = TWO_PI / period * (product % period).astype(jnp.float32)
    return (jnp.cos(angle), jnp.sin(angle))


def inverse_transform(spec_re, spec_im):
    full_length = OUTER_FACTOR * INNER_FACTOR
    leading = spec_re.shape[:-1]
    block_re = spec_re.reshape(leading + (OUTER_FACTOR, INNER_FACTOR))
    block_im = spec_im.reshape(leading + (OUTER_FACTOR, INNER_FACTOR))
    index_outer = jnp.arange(OUTER_FACTOR, dtype=jnp.int32)
    index_inner = jnp.arange(INNER_FACTOR, dtype=jnp.int32)
    cos_outer, sin_outer = phase_table(index_outer[:, None] * index_outer[None, :], OUTER_FACTOR)
    first_re = jnp.einsum('nb,...bq->...nq', cos_outer, block_re, precision=HIGHEST) - jnp.einsum('nb,...bq->...nq', sin_outer, block_im, precision=HIGHEST)
    first_im = jnp.einsum('nb,...bq->...nq', cos_outer, block_im, precision=HIGHEST) + jnp.einsum('nb,...bq->...nq', sin_outer, block_re, precision=HIGHEST)
    cos_twist, sin_twist = phase_table(index_outer[:, None] * index_inner[None, :], full_length)
    twist_re = first_re * cos_twist - first_im * sin_twist
    twist_im = first_re * sin_twist + first_im * cos_twist
    cos_inner, sin_inner = phase_table(index_inner[:, None] * index_inner[None, :], INNER_FACTOR)
    final_re = jnp.einsum('...nq,qm->...mn', twist_re, cos_inner, precision=HIGHEST) - jnp.einsum('...nq,qm->...mn', twist_im, sin_inner, precision=HIGHEST)
    final_im = jnp.einsum('...nq,qm->...mn', twist_re, sin_inner, precision=HIGHEST) + jnp.einsum('...nq,qm->...mn', twist_im, cos_inner, precision=HIGHEST)
    normalizer = 1.0 / math.sqrt(full_length)
    return (final_re.reshape(leading + (full_length,)) * normalizer, final_im.reshape(leading + (full_length,)) * normalizer)


def echo_response(key, salt, weakest, strongest, bin_index):
    full_length = OUTER_FACTOR * INNER_FACTOR
    delays = jax.random.randint(jax.random.fold_in(key, salt), (CH,), 3 * full_length // 16, 7 * full_length // 16, dtype=jnp.int32)
    log_strength = jax.random.uniform(jax.random.fold_in(key, salt + 1), (CH,), jnp.float32, math.log(weakest), math.log(strongest))
    strength = jnp.exp(log_strength)
    phase_angle = jax.random.uniform(jax.random.fold_in(key, salt + 2), (CH,), jnp.float32, -math.pi, math.pi)
    cos_delay, sin_delay = phase_table(bin_index[None, :] * delays[:, None], full_length)
    turn_re = jnp.cos(phase_angle)[:, None] * cos_delay + jnp.sin(phase_angle)[:, None] * sin_delay
    turn_im = jnp.sin(phase_angle)[:, None] * cos_delay - jnp.cos(phase_angle)[:, None] * sin_delay
    return (strength[:, None] * turn_re, strength[:, None] * turn_im)


def draw_samples(key, part):
    full_length = OUTER_FACTOR * INNER_FACTOR
    lower_edge = (full_length - ACTIVE_TONES) // 2
    symbol_index = decoded_levels(key)
    starts = window_starts(key)
    level_re = (2 * (symbol_index % 8) - 7).astype(jnp.float32) / math.sqrt(42.0)
    level_im = (2 * (symbol_index // 8) - 7).astype(jnp.float32) / math.sqrt(42.0)
    padding = ((0, 0), (lower_edge, full_length - ACTIVE_TONES - lower_edge))
    data_re = jnp.pad(level_re, padding)
    data_im = jnp.pad(level_im, padding)
    bin_index = jnp.arange(full_length, dtype=jnp.int32)
    chan_re, chan_im = echo_response(key, 303, 1.5, 3.0, bin_index)
    spec_re = data_re[None] * chan_re[:, None] - data_im[None] * chan_im[:, None]
    spec_im = data_re[None] * chan_im[:, None] + data_im[None] * chan_re[:, None]
    wave_re, wave_im = inverse_transform(spec_re, spec_im)
    noise_key = jax.random.fold_in(key, 505)
    noise_part = 0.15 * jax.random.normal(noise_key, (2, CH, SYMBOL_COUNT, full_length), jnp.float32)
    waveform = jnp.stack([wave_re, wave_im]) + noise_part
    places = jnp.arange(full_length + GUARD_SAMPLES, dtype=jnp.int32)
    source = (places[None, :] - starts[:, None]) % full_length
    gather_index = jnp.broadcast_to(source[None, None], (2, CH, SYMBOL_COUNT, full_length + GUARD_SAMPLES))
    picked = jnp.take_along_axis(waveform, gather_index, axis=3)
    return jnp.clip(picked, -16.0, 16.0).astype(jnp.float32)


def plant(array, own_key, low, largest):
    index_at = [jax.random.randint(jax.random.fold_in(own_key, axis), (), 0, length) for axis, length in enumerate(array.shape)]
    main_axis = array.shape.index(max(array.shape))
    next_to = index_at[:main_axis] + [(index_at[main_axis] + 1) % array.shape[main_axis]] + index_at[main_axis + 1:]
    return array.at[tuple(index_at)].set(low).at[tuple(next_to)].set(largest)


def setup_inputs(seed: int = 0, part: int = 0) -> dict:
    keys = jax.random.split(jax.random.key(seed), 5)
    part_keys = jax.random.split(jax.random.fold_in(keys[4], part), 5)
    return {
        "samples": draw_samples(jax.random.fold_in(jax.random.fold_in(keys[4], part), 71), part),
        "constellation_index": draw_constellation_index(jax.random.fold_in(jax.random.fold_in(keys[4], part), 71), part),
        "pilot_offsets": plant(jax.random.randint(keys[2], (SYMBOL_COUNT,), 0, PSP), jax.random.fold_in(keys[2], 1), 0, PSP - 1).astype(jnp.int32),
        "cp_offset": draw_cp_offset(jax.random.fold_in(jax.random.fold_in(keys[4], part), 71), part),
    }


def reference(samples, constellation_index, pilot_offsets, cp_offset):
    grand_total = OUTER_FACTOR * INNER_FACTOR

    def one_symbol(record, offset):
        return lax.dynamic_slice_in_dim(record, offset.astype(jnp.int32), grand_total, axis=2)
    symbol_windows = jax.vmap(one_symbol, in_axes=(2, 0), out_axes=2)(samples, cp_offset)
    symbol_spectrum = jnp.fft.fft(symbol_windows[0] + 1j * symbol_windows[1], axis=-1) / math.sqrt(grand_total)
    lower_edge = (grand_total - ACTIVE_TONES) // 2
    band_slice = symbol_spectrum[..., lower_edge:lower_edge + ACTIVE_TONES]
    level_real = (2 * (constellation_index % 8) - 7).astype(jnp.float32)
    level_imaginary = (2 * (constellation_index // 8) - 7).astype(jnp.float32)
    factor = math.sqrt(42.0) / (level_real * level_real + level_imaginary * level_imaginary)
    ratio_re = (jnp.real(band_slice) * level_real + jnp.imag(band_slice) * level_imaginary) * factor
    ratio_im = (jnp.imag(band_slice) * level_real - jnp.real(band_slice) * level_imaginary) * factor
    ratio = jnp.stack([ratio_re, ratio_im])
    positions = jnp.arange(ACTIVE_TONES, dtype=jnp.int32)
    pilot = (positions[None, :] % PSP == pilot_offsets[:, None]).astype(jnp.float32)
    values = ratio * pilot
    zero_padded = jnp.pad(values, ((0, 0), (0, 0), (0, 0), (SMOOTH_HALFSPAN, SMOOTH_HALFSPAN)))
    pilot_padded = jnp.pad(pilot, ((0, 0), (SMOOTH_HALFSPAN, SMOOTH_HALFSPAN)))
    numerator = jnp.zeros(values.shape, jnp.float32)
    denominator = jnp.zeros(pilot.shape, jnp.float32)
    for shift_amount in range(-SMOOTH_HALFSPAN, SMOOTH_HALFSPAN + 1):
        taper_weight = float(SMOOTH_HALFSPAN + 1 - abs(shift_amount))
        numerator = numerator + taper_weight * zero_padded[..., SMOOTH_HALFSPAN + shift_amount:SMOOTH_HALFSPAN + shift_amount + ACTIVE_TONES]
        denominator = denominator + taper_weight * pilot_padded[:, SMOOTH_HALFSPAN + shift_amount:SMOOTH_HALFSPAN + shift_amount + ACTIVE_TONES]
    purified = ratio - numerator / denominator
    delay_profile = jnp.fft.ifft(purified[0] + 1j * purified[1], axis=-1)[..., :GUARD_SAMPLES] * math.sqrt(ACTIVE_TONES)
    spread = jnp.fft.fft(delay_profile, axis=1) / math.sqrt(delay_profile.shape[1])
    return jnp.stack([jnp.real(spread), jnp.imag(spread)]).astype(jnp.float32)
```

```python
import functools
import math

import jax
import jax.numpy as jnp
import ml_dtypes
import numpy as np
from jax import lax
from jax.experimental import pallas as pl
from jax.experimental.pallas import tpu as pltpu
from jax.sharding import PartitionSpec as P

MESH = pl.DeviceIdType.MESH
BF16 = jnp.bfloat16
F32 = jnp.float32

LENGTH = 8192
TONES = 4096
LOWEST = 2048
RADIX = 32
LANES = 128
GUARD = 1024
HALFSPAN = 48
PSP = 12
SYM = 4
SUB = 16
MS = 6
SYMBOLS = 24
SHIFTS = (-2, -1, 0, 1, 2)


def halves(matrix):
    high = matrix.astype(ml_dtypes.bfloat16)
    low = (matrix - high.astype(np.float64)).astype(ml_dtypes.bfloat16)
    return high, low


def tables():
    p = np.arange(RADIX)
    turn = 2.0 * np.pi
    c = np.cos(turn * np.outer(p, p) / RADIX)
    s = np.sin(turn * np.outer(p, p) / RADIX)
    high, low = halves(np.block([[c, s], [-s, c]]))
    first = np.concatenate([high, low, high], axis=1)
    b = np.arange(256)
    angle = turn * np.outer(p, b) / LENGTH
    twist = np.stack([np.cos(angle), np.sin(angle)]).astype(np.float32)
    j = LOWEST // RADIX + np.arange(LANES)
    angle = turn * (np.outer(b, j) % 256) / 256
    c, s = np.cos(angle), np.sin(angle)
    second = np.stack(halves(np.block([[c, -s], [s, c]]) / math.sqrt(LENGTH)))
    rows = []
    for shift in SHIFTS:
        gap = RADIX * shift + p[None, :] - p[:, None]
        rows.append(np.maximum(HALFSPAN + 1 - np.abs(gap), 0))
    taper = np.concatenate(rows, axis=0)
    taper = np.concatenate([taper, taper], axis=1).astype(ml_dtypes.bfloat16)
    v = np.arange(LANES)
    angle = turn * (np.outer(v, v) % LANES) / LANES
    c, s = np.cos(angle), np.sin(angle)
    third = np.stack(halves(np.block([[c, s], [-s, c]]) / math.sqrt(TONES * SYMBOLS)))
    angle = turn * np.outer(p, v) / TONES
    twirl = np.stack([np.cos(angle), np.sin(angle)]).astype(np.float32)
    u = np.arange(GUARD // LANES)
    angle = turn * (np.outer(u, p) % RADIX) / RADIX
    c, s = np.cos(angle), np.sin(angle)
    high, low = halves(np.block([[c, -s], [s, c]]))
    fourth = np.concatenate([high, low, high], axis=1)
    spread = np.zeros((4, RADIX, LANES), ml_dtypes.bfloat16)
    for g in range(4):
        spread[g, p, 4 * p + g] = 1
    doppler = np.zeros((SYM, 16, 64), np.float64)
    for block in range(SYM):
        for f in range(MS):
            for source in range(SYM):
                for m in range(MS):
                    angle = turn * (((MS * source + m) * (MS * block + f)) % SYMBOLS) / SYMBOLS
                    doppler[block, f, 8 * source + m] = np.cos(angle)
                    doppler[block, f, 32 + 8 * source + m] = np.sin(angle)
    high, low = halves(doppler)
    doppler = np.concatenate([high, low, high], axis=2)
    return first, twist, second, taper, third, twirl, fourth, spread, doppler


def dot(a, b):
    return jnp.dot(a, b, preferred_element_type=F32)


def parted(value):
    high = value.astype(BF16)
    low = (value - high.astype(F32)).astype(BF16)
    return high, low


def kernel(
    cp_ref,
    pilot_ref,
    x_hbm,
    index_ref,
    first_ref,
    twist_ref,
    second_ref,
    taper_ref,
    third_ref,
    twirl_ref,
    fourth_ref,
    spread_ref,
    doppler_ref,
    out_ref,
    x_ref,
    y_ref,
    zh_ref,
    zl_ref,
    itmp_ref,
    isend_ref,
    igath_ref,
    ig_ref,
    send_ref,
    recv_ref,
    x_sem,
    isend_sem,
    irecv_sem,
    send_sem,
    recv_sem,
    ready_sem,
):
    sym = lax.axis_index("sym")
    sub = lax.axis_index("sub")
    barrier = pltpu.get_barrier_semaphore()

    load = pltpu.make_async_copy(x_hbm.at[:, 0], x_ref, x_sem)
    load.start()

    for d in range(1, SUB):
        pl.semaphore_signal(
            barrier, inc=1, device_id={"sub": lax.rem(sub + d, SUB)}, device_id_type=MESH
        )
    for d in range(1, SYM):
        pl.semaphore_signal(
            barrier, inc=1, device_id={"sym": lax.rem(sym + d, SYM)}, device_id_type=MESH
        )

    itmp_ref[...] = jnp.zeros_like(itmp_ref)
    index = index_ref[...].astype(F32)
    itmp_ref[0:MS, :] = index[:, :LANES]
    itmp_ref[8 : 8 + MS, :] = index[:, LANES:]
    isend_ref[...] = itmp_ref[...].astype(BF16)
    send_ref[...] = jnp.zeros_like(send_ref)

    lane = lax.broadcasted_iota(jnp.int32, (RADIX, LANES), 1)
    row = lax.broadcasted_iota(jnp.int32, (RADIX, LANES), 0)
    start_lanes = jnp.zeros((RADIX, LANES), jnp.int32)
    row8 = lax.broadcasted_iota(jnp.int32, (8, LANES), 0)
    lane8 = lax.broadcasted_iota(jnp.int32, (8, LANES), 1)
    start_rows = jnp.zeros((8, LANES), jnp.int32)
    for m in range(MS):
        start_lanes = jnp.where(lane == m, cp_ref[m], start_lanes)
        start_rows = jnp.where(row8 == m, cp_ref[m], start_rows)
    step = 2.0 * math.pi / LENGTH
    angle = ((start_lanes * row) & (LENGTH - 1)).astype(F32) * step
    row_cos, row_sin = jnp.cos(angle), jnp.sin(angle)
    angle = ((start_rows * (LOWEST + RADIX * lane8)) & (LENGTH - 1)).astype(F32) * step
    lane_cos, lane_sin = jnp.cos(angle), jnp.sin(angle)
    residue = lax.rem(RADIX * lane + row, PSP)

    load.wait()
    lane6 = lax.broadcasted_iota(jnp.int32, (MS, LANES), 1)
    starts = start_rows[0:MS]
    for part in range(2):
        for t in range(LENGTH // LANES):
            value = x_ref[part, :, pl.ds(t * LANES, LANES)]
            if t * LANES < GUARD:
                later = x_ref[part, :, pl.ds(LENGTH + t * LANES, LANES)]
                value = jnp.where(lane6 + t * LANES >= starts, value, later)
            y_ref[t % 2, pl.ds(part * RADIX + t // 2, MS, stride=64), :] = value

    twist_cos, twist_sin = twist_ref[0], twist_ref[1]
    for m in range(MS):
        value = jnp.concatenate(
            [y_ref[0, pl.ds(64 * m, 64), :], y_ref[1, pl.ds(64 * m, 64), :]], axis=1
        )
        high, low = parted(value)
        y = dot(first_ref[...], jnp.concatenate([high, high, low], axis=0))
        re, im = y[:RADIX], y[RADIX:]
        z = jnp.concatenate(
            [re * twist_cos + im * twist_sin, im * twist_cos - re * twist_sin], axis=1
        )
        high, low = parted(z)
        zh_ref[pl.ds(RADIX * m, RADIX), :] = high
        zl_ref[pl.ds(RADIX * m, RADIX), :] = low

    pl.semaphore_wait(barrier, SUB + SYM - 2)
    mine = pl.ds(pl.multiple_of(16 * sub, 16), 16)
    for d in range(1, SUB):
        pltpu.make_async_remote_copy(
            src_ref=isend_ref,
            dst_ref=igath_ref.at[mine],
            send_sem=isend_sem,
            recv_sem=irecv_sem,
            device_id={"sub": lax.rem(sub + d, SUB)},
            device_id_type=MESH,
        ).start()
    for d in range(1, SYM):
        pl.semaphore_signal(
            ready_sem, inc=1, device_id={"sym": lax.rem(sym + d, SYM)}, device_id_type=MESH
        )
    igath_ref[mine, :] = isend_ref[...]

    zh = zh_ref[...]
    spectra = dot(zh, second_ref[0]) + dot(zl_ref[...], second_ref[0]) + dot(zh, second_ref[1])

    all_index = igath_ref.at[pl.ds(0, 16 * (SUB - 1))]
    pltpu.make_async_remote_copy(
        src_ref=all_index,
        dst_ref=all_index,
        send_sem=isend_sem,
        recv_sem=irecv_sem,
        device_id={"sub": lax.rem(sub + 1, SUB)},
        device_id_type=MESH,
    ).wait()
    ig_ref[...] = igath_ref[...].astype(F32)

    natural = [jnp.transpose(ig_ref[pl.ds(m, RADIX, stride=8), :]) for m in range(MS)]
    natural = [value.astype(BF16) for value in natural]
    index = sum(
        dot(
            jnp.concatenate([value[RADIX * g : RADIX * (g + 1)] for value in natural], axis=0),
            spread_ref[g],
        )
        for g in range(4)
    )

    high_rows, low_rows = [], []
    for m in range(MS):
        rows = slice(RADIX * m, RADIX * (m + 1))
        quadrature = jnp.floor(index[rows] * 0.125)
        level_re = 2.0 * (index[rows] - 8.0 * quadrature) - 7.0
        level_im = 2.0 * quadrature - 7.0
        factor = math.sqrt(42.0) / (level_re * level_re + level_im * level_im)
        lc = lane_cos[m : m + 1, :]
        ls = lane_sin[m : m + 1, :]
        rc = jnp.broadcast_to(row_cos[:, m : m + 1], (RADIX, LANES))
        rs = jnp.broadcast_to(row_sin[:, m : m + 1], (RADIX, LANES))
        phase_re = (lc * rc - ls * rs) * factor
        phase_im = (lc * rs + ls * rc) * factor
        gain_re = phase_re * level_re + phase_im * level_im
        gain_im = phase_im * level_re - phase_re * level_im
        re, im = spectra[rows, :LANES], spectra[rows, LANES:]
        ratio_re = re * gain_re - im * gain_im
        ratio_im = re * gain_im + im * gain_re
        ratio = jnp.concatenate([ratio_re, ratio_im], axis=1)
        pilot = (residue == pilot_ref[m]).astype(F32)
        high, low = parted(ratio * jnp.concatenate([pilot, pilot], axis=1))
        right = jnp.concatenate(
            [
                jnp.concatenate([high, pilot.astype(BF16)], axis=1),
                jnp.concatenate([low, jnp.zeros((RADIX, LANES), BF16)], axis=1),
            ],
            axis=0,
        )
        tapered = dot(taper_ref[...], right)
        sums = []
        for part in range(3):
            total = None
            for i, shift in enumerate(SHIFTS):
                term = tapered[RADIX * i : RADIX * (i + 1), LANES * part : LANES * (part + 1)]
                if shift:
                    term = pltpu.roll(term, (-shift) % LANES, 1)
                    inside = lane < LANES - shift if shift > 0 else lane >= -shift
                    term = jnp.where(inside, term, 0.0)
                total = term if total is None else total + term
            sums.append(total)
        inverse = 1.0 / sums[2]
        cleaned = jnp.concatenate(
            [ratio_re - sums[0] * inverse, ratio_im - sums[1] * inverse], axis=1
        )
        high, low = parted(cleaned)
        high_rows.append(high)
        low_rows.append(low)
    high = jnp.concatenate(high_rows, axis=0)
    low = jnp.concatenate(low_rows, axis=0)
    folded = dot(high, third_ref[0]) + dot(low, third_ref[0]) + dot(high, third_ref[1])

    twirl_cos, twirl_sin = twirl_ref[0], twirl_ref[1]
    columns = []
    for m in range(MS):
        rows = slice(RADIX * m, RADIX * (m + 1))
        re, im = folded[rows, :LANES], folded[rows, LANES:]
        value = jnp.concatenate(
            [re * twirl_cos - im * twirl_sin, re * twirl_sin + im * twirl_cos], axis=0
        )
        high, low = parted(value)
        columns.append(jnp.concatenate([high, high, low], axis=0))
    profile = dot(fourth_ref[...], jnp.concatenate(columns, axis=1))
    for m in range(MS):
        re = profile[0:8, LANES * m : LANES * (m + 1)]
        im = profile[8:16, LANES * m : LANES * (m + 1)]
        send_ref[0, pl.ds(m, 8, stride=8), :] = jnp.where(lane8 < 64, re, pltpu.roll(im, 64, 1))
        send_ref[1, pl.ds(m, 8, stride=8), :] = jnp.where(lane8 < 64, pltpu.roll(re, 64, 1), im)

    pl.semaphore_wait(ready_sem, SYM - 1)
    slot = pl.ds(pl.multiple_of(8 * (SYM * sub + sym), 8), 8)

    def block(to_sub):
        return send_ref.at[lax.rem(to_sub, 2), pl.ds(pl.multiple_of(8 * (to_sub // 2), 8), 8)]

    for e in (2, 1, 3, 0):
        for d in range(SUB):
            if e == 0 and d == 0:
                continue
            to_sub = lax.rem(sub + d, SUB)
            pltpu.make_async_remote_copy(
                src_ref=block(to_sub),
                dst_ref=recv_ref.at[slot],
                send_sem=send_sem,
                recv_sem=recv_sem,
                device_id={"sym": lax.rem(sym + e, SYM), "sub": to_sub},
                device_id_type=MESH,
            ).start()
    recv_ref[slot, :] = send_ref[lax.rem(sub, 2), pl.ds(pl.multiple_of(8 * (sub // 2), 8), 8), :]

    everything = recv_ref.at[pl.ds(0, 8 * (SYM * SUB - 1))]
    pltpu.make_async_remote_copy(
        src_ref=everything,
        dst_ref=everything,
        send_sem=send_sem,
        recv_sem=recv_sem,
        device_id={"sub": lax.rem(sub + 1, SUB)},
        device_id_type=MESH,
    ).wait()

    columns = []
    for c in range(SUB):
        value = recv_ref[pl.ds(32 * c, 32), :]
        turned = pltpu.roll(value, 64, 1)
        turned = jnp.where(lane < 64, turned, -turned)
        high, low = parted(jnp.concatenate([value, turned], axis=0))
        columns.append(jnp.concatenate([high, high, low], axis=0))
    result = dot(doppler_ref[sym], jnp.concatenate(columns, axis=1))
    for c in range(SUB):
        value = result[0:8, LANES * c : LANES * (c + 1)]
        out_ref[0, c, :, :] = value[0:MS, 0:64]
        out_ref[1, c, :, :] = pltpu.roll(value, 64, 1)[0:MS, 0:64]


def body(samples, constellation_index, pilot_offsets, cp_offset):
    consts = [jnp.asarray(table) for table in tables()]
    smem = pl.BlockSpec(memory_space=pltpu.SMEM)
    vmem = pl.BlockSpec(memory_space=pltpu.VMEM)
    hbm = pl.BlockSpec(memory_space=pl.ANY)
    return pl.pallas_call(
        kernel,
        out_shape=jax.ShapeDtypeStruct((2, SUB, MS, GUARD // SUB), F32),
        in_specs=[smem, smem, hbm] + [vmem] * (1 + len(consts)),
        out_specs=vmem,
        scratch_shapes=[
            pltpu.VMEM((2, MS, LENGTH + GUARD), F32),
            pltpu.VMEM((2, 64 * MS, LANES), F32),
            pltpu.VMEM((RADIX * MS, 512), BF16),
            pltpu.VMEM((RADIX * MS, 512), BF16),
            pltpu.VMEM((16, LANES), F32),
            pltpu.VMEM((16, LANES), BF16),
            pltpu.VMEM((16 * SUB, LANES), BF16),
            pltpu.VMEM((16 * SUB, LANES), F32),
            pltpu.VMEM((2, 64, LANES), F32),
            pltpu.VMEM((8 * SYM * SUB, LANES), F32),
            pltpu.SemaphoreType.DMA,
            pltpu.SemaphoreType.DMA,
            pltpu.SemaphoreType.DMA,
            pltpu.SemaphoreType.DMA,
            pltpu.SemaphoreType.DMA,
            pltpu.SemaphoreType.REGULAR,
        ],
        compiler_params=pltpu.CompilerParams(collective_id=0, has_side_effects=True),
    )(cp_offset, pilot_offsets, samples, constellation_index, *consts)


def solution(mesh):
    return jax.shard_map(
        body,
        mesh=mesh,
        in_specs=(
            P(None, ("chan", "sub"), "sym", None),
            P(("chan", "sym"), "sub"),
            P("sym"),
            P(("chan", "sym")),
        ),
        out_specs=P(None, "chan", "sym", "sub"),
        check_vma=False,
    )
```

```python
import functools
import math

import jax
import jax.numpy as jnp
import ml_dtypes
import numpy as np
from jax import lax
from jax.experimental import pallas as pl
from jax.experimental.pallas import tpu as pltpu
from jax.sharding import PartitionSpec as P

MESH = pl.DeviceIdType.MESH
BF16 = jnp.bfloat16
F32 = jnp.float32

LENGTH = 8192
TONES = 4096
LOWEST = 2048
RADIX = 32
LANES = 128
GUARD = 1024
HALFSPAN = 48
PSP = 12
SYM = 4
SUB = 16
MS = 6
SYMBOLS = 24
SHIFTS = (-2, -1, 0, 1, 2)


def halves(matrix):
    high = matrix.astype(ml_dtypes.bfloat16)
    low = (matrix - high.astype(np.float64)).astype(ml_dtypes.bfloat16)
    return high, low


def tables():
    p = np.arange(RADIX)
    turn = 2.0 * np.pi
    c = np.cos(turn * np.outer(p, p) / RADIX)
    s = np.sin(turn * np.outer(p, p) / RADIX)
    high, low = halves(np.block([[c, s], [-s, c]]))
    first = np.concatenate([high, low, high], axis=1)
    b = np.arange(256)
    angle = turn * np.outer(p, b) / LENGTH
    twist = np.stack([np.cos(angle), np.sin(angle)]).astype(np.float32)
    j = LOWEST // RADIX + np.arange(LANES)
    angle = turn * (np.outer(b, j) % 256) / 256
    c, s = np.cos(angle), np.sin(angle)
    second = np.stack(halves(np.block([[c, -s], [s, c]]) / math.sqrt(LENGTH)))
    rows = []
    for shift in SHIFTS:
        gap = RADIX * shift + p[None, :] - p[:, None]
        rows.append(np.maximum(HALFSPAN + 1 - np.abs(gap), 0))
    taper = np.concatenate(rows, axis=0)
    taper = np.concatenate([taper, taper], axis=1).astype(ml_dtypes.bfloat16)
    v = np.arange(LANES)
    angle = turn * (np.outer(v, v) % LANES) / LANES
    c, s = np.cos(angle), np.sin(angle)
    third = np.stack(halves(np.block([[c, s], [-s, c]]) / math.sqrt(TONES * SYMBOLS)))
    angle = turn * np.outer(p, v) / TONES
    twirl = np.stack([np.cos(angle), np.sin(angle)]).astype(np.float32)
    u = np.arange(GUARD // LANES)
    angle = turn * (np.outer(u, p) % RADIX) / RADIX
    c, s = np.cos(angle), np.sin(angle)
    high, low = halves(np.block([[c, -s], [s, c]]))
    fourth = np.concatenate([high, low, high], axis=1)
    spread = np.zeros((4, RADIX, LANES), ml_dtypes.bfloat16)
    for g in range(4):
        for half in range(2):
            for owner in range(SUB):
                spread[g, SUB * half + owner, 4 * (2 * owner + half) + g] = 1
    f, m = np.arange(MS), np.arange(SYMBOLS)
    doppler = np.zeros((SYM, 2, MS, SYMBOLS), np.float32)
    for block in range(SYM):
        angle = turn * (np.outer(MS * block + f, m) % SYMBOLS) / SYMBOLS
        doppler[block] = np.cos(angle), np.sin(angle)
    doppler = doppler.reshape(SYM, 2 * MS * SYMBOLS)
    return first, twist, second, taper, third, twirl, fourth, spread, doppler


def dot(a, b):
    return jnp.dot(a, b, preferred_element_type=F32)


def parted(value):
    high = value.astype(BF16)
    low = (value - high.astype(F32)).astype(BF16)
    return high, low


RECORD = 72


def kernel(
    cp_hbm,
    pilot_hbm,
    x_hbm,
    index_hbm,
    first_hbm,
    twist_hbm,
    second_hbm,
    taper_hbm,
    third_hbm,
    twirl_hbm,
    fourth_hbm,
    spread_hbm,
    doppler_hbm,
    out_ref,
    cp_ref,
    pilot_ref,
    x_ref,
    index_ref,
    first_ref,
    twist_ref,
    second_ref,
    taper_ref,
    third_ref,
    twirl_ref,
    fourth_ref,
    spread_ref,
    doppler_ref,
    zh_ref,
    zl_ref,
    isend_ref,
    igath_ref,
    ig_ref,
    stage_ref,
    send_ref,
    recv_ref,
    got_ref,
    load_sem,
    isend_sem,
    irecv_sem,
    send_sem,
    recv_sem,
    near_sem,
    far_sem,
):
    sym = lax.axis_index("sym")
    sub = lax.axis_index("sub")
    barrier = pltpu.get_barrier_semaphore()
    before, after = lax.rem(sym + SYM - 1, SYM), lax.rem(sym + 1, SYM)

    for d in range(1, SUB):
        pl.semaphore_signal(
            barrier, inc=1, device_id={"sub": lax.rem(sub + d, SUB)}, device_id_type=MESH
        )
    for to in (before, after):
        pl.semaphore_signal(barrier, inc=1, device_id={"sym": to}, device_id_type=MESH)

    loads = [
        pltpu.make_async_copy(source, target, load_sem.at[i])
        for i, (source, target) in enumerate(
            (
                (index_hbm, index_ref),
                (cp_hbm, cp_ref),
                (x_hbm, x_ref),
                (first_hbm, first_ref),
                (twist_hbm, twist_ref),
                (second_hbm, second_ref),
                (pilot_hbm, pilot_ref),
                (spread_hbm, spread_ref),
                (taper_hbm, taper_ref),
                (third_hbm, third_ref),
                (twirl_hbm, twirl_ref),
                (fourth_hbm, fourth_ref),
                (doppler_hbm.at[pl.ds(sym, 1)], doppler_ref),
            )
        )
    ]
    for load in loads:
        load.start()

    lane = lax.broadcasted_iota(jnp.int32, (RADIX, LANES), 1)
    row = lax.broadcasted_iota(jnp.int32, (RADIX, LANES), 0)
    row8 = lax.broadcasted_iota(jnp.int32, (8, LANES), 0)
    lane8 = lax.broadcasted_iota(jnp.int32, (8, LANES), 1)
    residue = lax.rem(RADIX * lane + row, PSP)

    loads[0].wait()
    index = index_ref[...].astype(F32)
    isend_ref[...] = jnp.concatenate([index[:, :LANES], index[:, LANES:]], axis=0).astype(BF16)

    pl.semaphore_wait(barrier, SUB + 1)
    for d in (8, 9, 10, 11, 7, 6, 5, 4, 12, 13, 14, 15, 3, 2, 1):
        pltpu.make_async_remote_copy(
            src_ref=isend_ref,
            dst_ref=igath_ref.at[sub],
            send_sem=isend_sem,
            recv_sem=irecv_sem,
            device_id={"sub": lax.rem(sub + d, SUB)},
            device_id_type=MESH,
        ).start()
    for to in (before, after):
        pl.semaphore_signal(near_sem, inc=1, device_id={"sym": to}, device_id_type=MESH)
    igath_ref[sub] = isend_ref[...]

    loads[1].wait()
    start_lanes = jnp.zeros((RADIX, LANES), jnp.int32)
    start_rows = jnp.zeros((8, LANES), jnp.int32)
    for m in range(MS):
        start_lanes = jnp.where(lane == m, cp_ref[m], start_lanes)
        start_rows = jnp.where(row8 == m, cp_ref[m], start_rows)
    step = 2.0 * math.pi / LENGTH
    angle = ((start_lanes * row) & (LENGTH - 1)).astype(F32) * step
    row_cos, row_sin = jnp.cos(angle), jnp.sin(angle)
    angle = ((start_rows * (LOWEST + RADIX * lane8)) & (LENGTH - 1)).astype(F32) * step
    lane_cos, lane_sin = jnp.cos(angle), jnp.sin(angle)

    for i in (2, 3, 4):
        loads[i].wait()
    place = LANES * row8 + lane8
    twist_cos, twist_sin = twist_ref[0], twist_ref[1]
    for m in range(MS):
        pieces = []
        for part in range(2):
            base = RECORD * (MS * part + m)
            x_ref[pl.ds(base, 8), :] = jnp.where(
                place >= cp_ref[m], x_ref[pl.ds(base, 8), :], x_ref[pl.ds(base + 64, 8), :]
            )
            pieces.append(
                jnp.concatenate(
                    [x_ref[pl.ds(base + i, RADIX, stride=2), :] for i in range(2)], axis=1
                )
            )
        high, low = parted(jnp.concatenate(pieces, axis=0))
        y = dot(first_ref[...], jnp.concatenate([high, high, low], axis=0))
        re, im = y[:RADIX], y[RADIX:]
        z = jnp.concatenate(
            [re * twist_cos + im * twist_sin, im * twist_cos - re * twist_sin], axis=1
        )
        high, low = parted(z)
        zh_ref[pl.ds(RADIX * m, RADIX), :] = high
        zl_ref[pl.ds(RADIX * m, RADIX), :] = low
    loads[5].wait()
    zh = zh_ref[...]
    spectra = dot(zh, second_ref[0]) + dot(zl_ref[...], second_ref[0]) + dot(zh, second_ref[1])

    for i in range(6, 13):
        loads[i].wait()
    pl.semaphore_wait(near_sem, 2)
    pl.semaphore_signal(far_sem, inc=1, device_id={"sym": before}, device_id_type=MESH)

    all_index = igath_ref.at[pl.ds(0, SUB - 1)]
    index_copies = pltpu.make_async_remote_copy(
        src_ref=all_index,
        dst_ref=all_index,
        send_sem=isend_sem,
        recv_sem=irecv_sem,
        device_id={"sub": lax.rem(sub + 1, SUB)},
        device_id_type=MESH,
    )
    index_copies.wait_recv()
    for owner in range(SUB):
        ig_ref[pl.ds(16 * owner, 2 * MS), :] = igath_ref[owner].astype(F32)

    natural = []
    for m in range(MS):
        value = jnp.concatenate(
            [ig_ref[pl.ds(MS * half + m, SUB, stride=16), :] for half in range(2)], axis=0
        )
        natural.append(jnp.transpose(value).astype(BF16))
    index = sum(
        dot(
            jnp.concatenate([value[RADIX * g : RADIX * (g + 1)] for value in natural], axis=0),
            spread_ref[g],
        )
        for g in range(4)
    )

    high_rows, low_rows = [], []
    for m in range(MS):
        rows = slice(RADIX * m, RADIX * (m + 1))
        quadrature = jnp.floor(index[rows] * 0.125)
        level_re = 2.0 * (index[rows] - 8.0 * quadrature) - 7.0
        level_im = 2.0 * quadrature - 7.0
        factor = math.sqrt(42.0) / (level_re * level_re + level_im * level_im)
        lc = lane_cos[m : m + 1, :]
        ls = lane_sin[m : m + 1, :]
        rc = jnp.broadcast_to(row_cos[:, m : m + 1], (RADIX, LANES))
        rs = jnp.broadcast_to(row_sin[:, m : m + 1], (RADIX, LANES))
        phase_re = (lc * rc - ls * rs) * factor
        phase_im = (lc * rs + ls * rc) * factor
        gain_re = phase_re * level_re + phase_im * level_im
        gain_im = phase_im * level_re - phase_re * level_im
        re, im = spectra[rows, :LANES], spectra[rows, LANES:]
        ratio_re = re * gain_re - im * gain_im
        ratio_im = re * gain_im + im * gain_re
        ratio = jnp.concatenate([ratio_re, ratio_im], axis=1)
        pilot = (residue == pilot_ref[m]).astype(F32)
        high, low = parted(ratio * jnp.concatenate([pilot, pilot], axis=1))
        right = jnp.concatenate(
            [
                jnp.concatenate([high, pilot.astype(BF16)], axis=1),
                jnp.concatenate([low, jnp.zeros((RADIX, LANES), BF16)], axis=1),
            ],
            axis=0,
        )
        tapered = dot(taper_ref[...], right)
        sums = []
        for part in range(3):
            total = None
            for i, shift in enumerate(SHIFTS):
                term = tapered[RADIX * i : RADIX * (i + 1), LANES * part : LANES * (part + 1)]
                if shift:
                    term = pltpu.roll(term, (-shift) % LANES, 1)
                    inside = lane < LANES - shift if shift > 0 else lane >= -shift
                    term = jnp.where(inside, term, 0.0)
                total = term if total is None else total + term
            sums.append(total)
        inverse = 1.0 / sums[2]
        cleaned = jnp.concatenate(
            [ratio_re - sums[0] * inverse, ratio_im - sums[1] * inverse], axis=1
        )
        high, low = parted(cleaned)
        high_rows.append(high)
        low_rows.append(low)
    high = jnp.concatenate(high_rows, axis=0)
    low = jnp.concatenate(low_rows, axis=0)
    folded = dot(high, third_ref[0]) + dot(low, third_ref[0]) + dot(high, third_ref[1])

    twirl_cos, twirl_sin = twirl_ref[0], twirl_ref[1]
    columns = []
    for m in range(MS):
        rows = slice(RADIX * m, RADIX * (m + 1))
        re, im = folded[rows, :LANES], folded[rows, LANES:]
        value = jnp.concatenate(
            [re * twirl_cos - im * twirl_sin, re * twirl_sin + im * twirl_cos], axis=0
        )
        high, low = parted(value)
        columns.append(jnp.concatenate([high, high, low], axis=0))
    profile = dot(fourth_ref[...], jnp.concatenate(columns, axis=1))

    pairs = []
    for m in range(MS):
        re = profile[0:8, LANES * m : LANES * (m + 1)]
        im = profile[8:16, LANES * m : LANES * (m + 1)]
        pairs.append(
            (
                jnp.where(lane8 < 64, re, pltpu.roll(im, 64, 1)),
                jnp.where(lane8 < 64, pltpu.roll(re, 64, 1), im),
            )
        )
    for half in range(2):
        largest = functools.reduce(jnp.maximum, [jnp.abs(pair[half]) for pair in pairs])
        largest = jnp.maximum(jnp.max(largest, axis=1, keepdims=True), 1e-30)
        code = jnp.broadcast_to(jnp.ceil(jnp.log2(largest) * 256.0), (8, LANES))
        inverse = 32767.0 * jnp.exp2(code * (-1.0 / 256.0))
        for m in range(MS):
            value = jnp.clip(jnp.round(pairs[m][half] * inverse), -32767.0, 32767.0)
            stage_ref[half, pl.ds(m, 8, stride=8), :] = value.astype(jnp.int32)
        stage_ref[half, pl.ds(MS, 8, stride=8), :] = code.astype(jnp.int32)
        stage_ref[half, pl.ds(MS + 1, 8, stride=8), :] = jnp.zeros((8, LANES), jnp.int32)
        for u in range(8):
            send_ref[2 * u + half] = stage_ref[half, pl.ds(8 * u, 8), :].astype(jnp.int16)

    pl.semaphore_wait(far_sem, 1)
    slot = SUB * sym + sub
    for e in (2, 1, 3, 0):
        for d in (8, 9, 10, 11, 7, 6, 5, 4, 12, 13, 14, 15, 3, 2, 1, 0):
            if e == 0 and d == 0:
                continue
            to_sub = lax.rem(sub + d, SUB)
            pltpu.make_async_remote_copy(
                src_ref=send_ref.at[to_sub],
                dst_ref=recv_ref.at[slot],
                send_sem=send_sem,
                recv_sem=recv_sem,
                device_id={"sym": lax.rem(sym + e, SYM), "sub": to_sub},
                device_id_type=MESH,
            ).start()
    recv_ref[slot] = send_ref[sub]

    everything = recv_ref.at[pl.ds(0, SYM * SUB - 1)]
    copies = pltpu.make_async_remote_copy(
        src_ref=everything,
        dst_ref=everything,
        send_sem=send_sem,
        recv_sem=recv_sem,
        device_id={"sub": lax.rem(sub + 1, SUB)},
        device_id_type=MESH,
    )
    copies.wait_recv()
    for i in range(SYM * SUB):
        got_ref[pl.ds(8 * i, 8), :] = recv_ref[i].astype(jnp.int32).astype(F32)

    cosines = [None] * MS
    sines = [None] * MS
    for s in range(SYM):
        base = 8 * SUB * s
        code = got_ref[pl.ds(base + MS, SUB, stride=8), :]
        scale = jnp.exp2(code * (1.0 / 256.0)) * (1.0 / 32767.0)
        for m in range(MS):
            value = got_ref[pl.ds(base + m, SUB, stride=8), :] * scale
            for f in range(MS):
                at = SYMBOLS * f + MS * s + m
                c = value * doppler_ref[0, at]
                n = value * doppler_ref[0, SYMBOLS * MS + at]
                cosines[f] = c if cosines[f] is None else cosines[f] + c
                sines[f] = n if sines[f] is None else sines[f] + n
    lane16 = lax.broadcasted_iota(jnp.int32, (SUB, LANES), 1)
    for f in range(MS):
        turned = pltpu.roll(sines[f], 64, 1)
        value = cosines[f] + jnp.where(lane16 < 64, turned, -turned)
        out_ref[0, f, :, :] = value[:, 0:64]
        out_ref[1, f, :, :] = pltpu.roll(value, 64, 1)[:, 0:64]

    index_copies.wait_send()
    copies.wait_send()


def body(samples, constellation_index, pilot_offsets, cp_offset):
    consts = [jnp.asarray(table) for table in tables()]
    vmem = pl.BlockSpec(memory_space=pltpu.VMEM)
    hbm = pl.BlockSpec(memory_space=pl.ANY)
    records = samples.reshape(2 * MS * RECORD, LANES)
    doppler = consts[-1]
    out = pl.pallas_call(
        kernel,
        out_shape=jax.ShapeDtypeStruct((2, MS, SUB, GUARD // SUB), F32),
        in_specs=[hbm] * (4 + len(consts)),
        out_specs=vmem,
        scratch_shapes=[
            pltpu.SMEM((MS,), jnp.int32),
            pltpu.SMEM((MS,), jnp.int32),
            pltpu.VMEM(records.shape, F32),
            pltpu.VMEM(constellation_index.shape, jnp.int32),
            *[pltpu.VMEM(table.shape, table.dtype) for table in consts[:-1]],
            pltpu.SMEM((1, doppler.shape[1]), F32),
            pltpu.VMEM((RADIX * MS, 512), BF16),
            pltpu.VMEM((RADIX * MS, 512), BF16),
            pltpu.VMEM((2 * MS, LANES), BF16),
            pltpu.VMEM((SUB, 2 * MS, LANES), BF16),
            pltpu.VMEM((16 * SUB, LANES), F32),
            pltpu.VMEM((2, 64, LANES), jnp.int32),
            pltpu.VMEM((SUB, 8, LANES), jnp.int16),
            pltpu.VMEM((SYM * SUB, 8, LANES), jnp.int16),
            pltpu.VMEM((8 * SYM * SUB, LANES), F32),
            pltpu.SemaphoreType.DMA((13,)),
            pltpu.SemaphoreType.DMA,
            pltpu.SemaphoreType.DMA,
            pltpu.SemaphoreType.DMA,
            pltpu.SemaphoreType.DMA,
            pltpu.SemaphoreType.REGULAR,
            pltpu.SemaphoreType.REGULAR,
        ],
        compiler_params=pltpu.CompilerParams(collective_id=0, has_side_effects=True),
    )(cp_offset, pilot_offsets, records, constellation_index, *consts)
    return out.transpose(0, 2, 1, 3)


def solution(mesh):
    return jax.shard_map(
        body,
        mesh=mesh,
        in_specs=(
            P(None, ("chan", "sub"), "sym", None),
            P(("chan", "sym"), "sub"),
            P("sym"),
            P(("chan", "sym")),
        ),
        out_specs=P(None, "chan", "sym", "sub"),
        check_vma=False,
    )
```

```python
import functools
import math

import jax
import jax.numpy as jnp
import ml_dtypes
import numpy as np
from jax import lax
from jax.experimental import pallas as pl
from jax.experimental.pallas import tpu as pltpu
from jax.sharding import PartitionSpec as P

MESH = pl.DeviceIdType.MESH
BF16 = jnp.bfloat16
F32 = jnp.float32

LENGTH = 8192
TONES = 4096
LOWEST = 2048
RADIX = 32
LANES = 128
GUARD = 1024
HALFSPAN = 48
PSP = 12
SYM = 4
SUB = 16
MS = 6
SYMBOLS = 24
SHIFTS = (-2, -1, 0, 1, 2)


def halves(matrix):
    high = matrix.astype(ml_dtypes.bfloat16)
    low = (matrix - high.astype(np.float64)).astype(ml_dtypes.bfloat16)
    return high, low


def tables():
    p = np.arange(RADIX)
    turn = 2.0 * np.pi
    c = np.cos(turn * np.outer(p, p) / RADIX)
    s = np.sin(turn * np.outer(p, p) / RADIX)
    high, low = halves(np.block([[c, s], [-s, c]]))
    first = np.concatenate([high, low, high], axis=1)
    b = np.arange(256)
    angle = turn * np.outer(p, b) / LENGTH
    twist = np.stack([np.cos(angle), np.sin(angle)]).astype(np.float32)
    j = LOWEST // RADIX + np.arange(LANES)
    angle = turn * (np.outer(b, j) % 256) / 256
    c, s = np.cos(angle), np.sin(angle)
    second = np.stack(halves(np.block([[c, -s], [s, c]]) / math.sqrt(LENGTH)))
    rows = []
    for shift in SHIFTS:
        gap = RADIX * shift + p[None, :] - p[:, None]
        rows.append(np.maximum(HALFSPAN + 1 - np.abs(gap), 0))
    taper = np.concatenate(rows, axis=0)
    taper = np.concatenate([taper, taper], axis=1).astype(ml_dtypes.bfloat16)
    v = np.arange(LANES)
    angle = turn * (np.outer(v, v) % LANES) / LANES
    c, s = np.cos(angle), np.sin(angle)
    third = np.stack(halves(np.block([[c, s], [-s, c]]) / math.sqrt(TONES * SYMBOLS)))
    angle = turn * np.outer(p, v) / TONES
    twirl = np.stack([np.cos(angle), np.sin(angle)]).astype(np.float32)
    u = np.arange(GUARD // LANES)
    angle = turn * (np.outer(u, p) % RADIX) / RADIX
    c, s = np.cos(angle), np.sin(angle)
    high, low = halves(np.block([[c, -s], [s, c]]))
    fourth = np.concatenate([high, low, high], axis=1)
    spread = np.zeros((4, RADIX, LANES), ml_dtypes.bfloat16)
    for g in range(4):
        for half in range(2):
            for owner in range(SUB):
                spread[g, SUB * half + owner, 4 * (2 * owner + half) + g] = 1
    f, m = np.arange(MS), np.arange(SYMBOLS)
    doppler = np.zeros((SYM, 2, MS, SYMBOLS), np.float32)
    for block in range(SYM):
        angle = turn * (np.outer(MS * block + f, m) % SYMBOLS) / SYMBOLS
        doppler[block] = np.cos(angle), np.sin(angle)
    doppler = doppler.reshape(SYM, 2 * MS * SYMBOLS)
    return first, twist, second, taper, third, twirl, fourth, spread, doppler


def dot(a, b):
    return jnp.dot(a, b, preferred_element_type=F32)


def parted(value):
    high = value.astype(BF16)
    low = (value - high.astype(F32)).astype(BF16)
    return high, low


RECORD = 72


def kernel(
    cp_hbm,
    pilot_hbm,
    x_hbm,
    index_hbm,
    first_hbm,
    twist_hbm,
    second_hbm,
    taper_hbm,
    third_hbm,
    twirl_hbm,
    fourth_hbm,
    spread_hbm,
    doppler_hbm,
    out_ref,
    cp_ref,
    pilot_ref,
    x_ref,
    index_ref,
    first_ref,
    twist_ref,
    second_ref,
    taper_ref,
    third_ref,
    twirl_ref,
    fourth_ref,
    spread_ref,
    doppler_ref,
    zh_ref,
    zl_ref,
    isend_ref,
    igath_ref,
    ig_ref,
    stage_ref,
    send_ref,
    recv_ref,
    got_ref,
    load_sem,
    isend_sem,
    irecv_sem,
    send_sem,
    recv_sem,
    near_sem,
    far_sem,
):
    sym = lax.axis_index("sym")
    sub = lax.axis_index("sub")
    barrier = pltpu.get_barrier_semaphore()
    before, after = lax.rem(sym + SYM - 1, SYM), lax.rem(sym + 1, SYM)

    for d in range(1, SUB):
        pl.semaphore_signal(
            barrier, inc=1, device_id={"sub": lax.rem(sub + d, SUB)}, device_id_type=MESH
        )
    for to in (before, after):
        pl.semaphore_signal(barrier, inc=1, device_id={"sym": to}, device_id_type=MESH)

    loads = [
        pltpu.make_async_copy(source, target, load_sem.at[i])
        for i, (source, target) in enumerate(
            (
                (index_hbm, index_ref),
                (cp_hbm, cp_ref),
                (x_hbm, x_ref),
                (first_hbm, first_ref),
                (twist_hbm, twist_ref),
                (second_hbm, second_ref),
                (pilot_hbm, pilot_ref),
                (spread_hbm, spread_ref),
                (taper_hbm, taper_ref),
                (third_hbm, third_ref),
                (twirl_hbm, twirl_ref),
                (fourth_hbm, fourth_ref),
                (doppler_hbm.at[pl.ds(sym, 1)], doppler_ref),
            )
        )
    ]
    for load in loads:
        load.start()

    lane = lax.broadcasted_iota(jnp.int32, (RADIX, LANES), 1)
    row = lax.broadcasted_iota(jnp.int32, (RADIX, LANES), 0)
    row8 = lax.broadcasted_iota(jnp.int32, (8, LANES), 0)
    lane8 = lax.broadcasted_iota(jnp.int32, (8, LANES), 1)
    residue = lax.rem(RADIX * lane + row, PSP)

    loads[0].wait()
    index = index_ref[...].astype(F32)
    isend_ref[...] = jnp.concatenate([index[:, :LANES], index[:, LANES:]], axis=0).astype(BF16)

    pl.semaphore_wait(barrier, SUB + 1)
    for d in (8, 9, 10, 11, 7, 6, 5, 4, 12, 13, 14, 15, 3, 2, 1):
        pltpu.make_async_remote_copy(
            src_ref=isend_ref,
            dst_ref=igath_ref.at[sub],
            send_sem=isend_sem,
            recv_sem=irecv_sem,
            device_id={"sub": lax.rem(sub + d, SUB)},
            device_id_type=MESH,
        ).start()
    for to in (before, after):
        pl.semaphore_signal(near_sem, inc=1, device_id={"sym": to}, device_id_type=MESH)
    igath_ref[sub] = isend_ref[...]

    loads[1].wait()
    start_lanes = jnp.zeros((RADIX, LANES), jnp.int32)
    start_rows = jnp.zeros((8, LANES), jnp.int32)
    for m in range(MS):
        start_lanes = jnp.where(lane == m, cp_ref[m], start_lanes)
        start_rows = jnp.where(row8 == m, cp_ref[m], start_rows)
    step = 2.0 * math.pi / LENGTH
    angle = ((start_lanes * row) & (LENGTH - 1)).astype(F32) * step
    row_cos, row_sin = jnp.cos(angle), jnp.sin(angle)
    angle = ((start_rows * (LOWEST + RADIX * lane8)) & (LENGTH - 1)).astype(F32) * step
    lane_cos, lane_sin = jnp.cos(angle), jnp.sin(angle)

    for i in (2, 3, 4):
        loads[i].wait()
    place = LANES * row8 + lane8
    twist_cos, twist_sin = twist_ref[0], twist_ref[1]
    for m in range(MS):
        pieces = []
        for part in range(2):
            base = RECORD * (MS * part + m)
            x_ref[pl.ds(base, 8), :] = jnp.where(
                place >= cp_ref[m], x_ref[pl.ds(base, 8), :], x_ref[pl.ds(base + 64, 8), :]
            )
            pieces.append(
                jnp.concatenate(
                    [x_ref[pl.ds(base + i, RADIX, stride=2), :] for i in range(2)], axis=1
                )
            )
        high, low = parted(jnp.concatenate(pieces, axis=0))
        y = dot(first_ref[...], jnp.concatenate([high, high, low], axis=0))
        re, im = y[:RADIX], y[RADIX:]
        z = jnp.concatenate(
            [re * twist_cos + im * twist_sin, im * twist_cos - re * twist_sin], axis=1
        )
        high, low = parted(z)
        zh_ref[pl.ds(RADIX * m, RADIX), :] = high
        zl_ref[pl.ds(RADIX * m, RADIX), :] = low
    loads[5].wait()
    zh = zh_ref[...]
    spectra = dot(zh, second_ref[0]) + dot(zl_ref[...], second_ref[0]) + dot(zh, second_ref[1])

    for i in range(6, 13):
        loads[i].wait()
    pl.semaphore_wait(near_sem, 2)
    pl.semaphore_signal(far_sem, inc=1, device_id={"sym": before}, device_id_type=MESH)

    all_index = igath_ref.at[pl.ds(0, SUB - 1)]
    index_copies = pltpu.make_async_remote_copy(
        src_ref=all_index,
        dst_ref=all_index,
        send_sem=isend_sem,
        recv_sem=irecv_sem,
        device_id={"sub": lax.rem(sub + 1, SUB)},
        device_id_type=MESH,
    )
    index_copies.wait_recv()
    for owner in range(SUB):
        ig_ref[pl.ds(16 * owner, 2 * MS), :] = igath_ref[owner].astype(F32)

    natural = []
    for m in range(MS):
        value = jnp.concatenate(
            [ig_ref[pl.ds(MS * half + m, SUB, stride=16), :] for half in range(2)], axis=0
        )
        natural.append(jnp.transpose(value).astype(BF16))
    index = sum(
        dot(
            jnp.concatenate([value[RADIX * g : RADIX * (g + 1)] for value in natural], axis=0),
            spread_ref[g],
        )
        for g in range(4)
    )

    high_rows, low_rows = [], []
    for m in range(MS):
        rows = slice(RADIX * m, RADIX * (m + 1))
        quadrature = jnp.floor(index[rows] * 0.125)
        level_re = 2.0 * (index[rows] - 8.0 * quadrature) - 7.0
        level_im = 2.0 * quadrature - 7.0
        factor = math.sqrt(42.0) / (level_re * level_re + level_im * level_im)
        lc = lane_cos[m : m + 1, :]
        ls = lane_sin[m : m + 1, :]
        rc = jnp.broadcast_to(row_cos[:, m : m + 1], (RADIX, LANES))
        rs = jnp.broadcast_to(row_sin[:, m : m + 1], (RADIX, LANES))
        phase_re = (lc * rc - ls * rs) * factor
        phase_im = (lc * rs + ls * rc) * factor
        gain_re = phase_re * level_re + phase_im * level_im
        gain_im = phase_im * level_re - phase_re * level_im
        re, im = spectra[rows, :LANES], spectra[rows, LANES:]
        ratio_re = re * gain_re - im * gain_im
        ratio_im = re * gain_im + im * gain_re
        ratio = jnp.concatenate([ratio_re, ratio_im], axis=1)
        pilot = (residue == pilot_ref[m]).astype(F32)
        high, low = parted(ratio * jnp.concatenate([pilot, pilot], axis=1))
        right = jnp.concatenate(
            [
                jnp.concatenate([high, pilot.astype(BF16)], axis=1),
                jnp.concatenate([low, jnp.zeros((RADIX, LANES), BF16)], axis=1),
            ],
            axis=0,
        )
        tapered = dot(taper_ref[...], right)
        sums = []
        for part in range(3):
            total = None
            for i, shift in enumerate(SHIFTS):
                term = tapered[RADIX * i : RADIX * (i + 1), LANES * part : LANES * (part + 1)]
                if shift:
                    term = pltpu.roll(term, (-shift) % LANES, 1)
                    inside = lane < LANES - shift if shift > 0 else lane >= -shift
                    term = jnp.where(inside, term, 0.0)
                total = term if total is None else total + term
            sums.append(total)
        inverse = 1.0 / sums[2]
        cleaned = jnp.concatenate(
            [ratio_re - sums[0] * inverse, ratio_im - sums[1] * inverse], axis=1
        )
        high, low = parted(cleaned)
        high_rows.append(high)
        low_rows.append(low)
    high = jnp.concatenate(high_rows, axis=0)
    low = jnp.concatenate(low_rows, axis=0)
    folded = dot(high, third_ref[0]) + dot(low, third_ref[0]) + dot(high, third_ref[1])

    twirl_cos, twirl_sin = twirl_ref[0], twirl_ref[1]
    columns = []
    for m in range(MS):
        rows = slice(RADIX * m, RADIX * (m + 1))
        re, im = folded[rows, :LANES], folded[rows, LANES:]
        value = jnp.concatenate(
            [re * twirl_cos - im * twirl_sin, re * twirl_sin + im * twirl_cos], axis=0
        )
        high, low = parted(value)
        columns.append(jnp.concatenate([high, high, low], axis=0))
    profile = dot(fourth_ref[...], jnp.concatenate(columns, axis=1))

    pairs = []
    for m in range(MS):
        re = profile[0:8, LANES * m : LANES * (m + 1)]
        im = profile[8:16, LANES * m : LANES * (m + 1)]
        pairs.append(
            (
                jnp.where(lane8 < 64, re, pltpu.roll(im, 64, 1)),
                jnp.where(lane8 < 64, pltpu.roll(re, 64, 1), im),
            )
        )
    for half in range(2):
        largest = functools.reduce(jnp.maximum, [jnp.abs(pair[half]) for pair in pairs])
        largest = jnp.maximum(jnp.max(largest, axis=1, keepdims=True), 1e-30)
        code = jnp.broadcast_to(jnp.ceil(jnp.log2(largest) * 256.0), (8, LANES))
        inverse = 32767.0 * jnp.exp2(code * (-1.0 / 256.0))
        for m in range(MS):
            value = jnp.clip(jnp.round(pairs[m][half] * inverse), -32767.0, 32767.0)
            stage_ref[half, pl.ds(m, 8, stride=8), :] = value.astype(jnp.int32)
        stage_ref[half, pl.ds(MS, 8, stride=8), :] = code.astype(jnp.int32)
        stage_ref[half, pl.ds(MS + 1, 8, stride=8), :] = jnp.zeros((8, LANES), jnp.int32)
        for u in range(8):
            send_ref[2 * u + half] = stage_ref[half, pl.ds(8 * u, 8), :].astype(jnp.int16)

    pl.semaphore_wait(far_sem, 1)
    slot = SUB * sym + sub
    for e in (2, 1, 3, 0):
        for d in (8, 9, 10, 11, 7, 6, 5, 4, 12, 13, 14, 15, 3, 2, 1, 0):
            if e == 0 and d == 0:
                continue
            to_sub = lax.rem(sub + d, SUB)
            pltpu.make_async_remote_copy(
                src_ref=send_ref.at[to_sub],
                dst_ref=recv_ref.at[slot],
                send_sem=send_sem,
                recv_sem=recv_sem,
                device_id={"sym": lax.rem(sym + e, SYM), "sub": to_sub},
                device_id_type=MESH,
            ).start()
    recv_ref[slot] = send_ref[sub]

    everything = recv_ref.at[pl.ds(0, SYM * SUB - 1)]
    copies = pltpu.make_async_remote_copy(
        src_ref=everything,
        dst_ref=everything,
        send_sem=send_sem,
        recv_sem=recv_sem,
        device_id={"sub": lax.rem(sub + 1, SUB)},
        device_id_type=MESH,
    )
    copies.wait_recv()
    for i in range(SYM * SUB):
        got_ref[pl.ds(8 * i, 8), :] = recv_ref[i].astype(jnp.int32).astype(F32)

    cosines = [None] * MS
    sines = [None] * MS
    for s in range(SYM):
        base = 8 * SUB * s
        code = got_ref[pl.ds(base + MS, SUB, stride=8), :]
        scale = jnp.exp2(code * (1.0 / 256.0)) * (1.0 / 32767.0)
        for m in range(MS):
            value = got_ref[pl.ds(base + m, SUB, stride=8), :] * scale
            for f in range(MS):
                at = SYMBOLS * f + MS * s + m
                c = value * doppler_ref[0, at]
                n = value * doppler_ref[0, SYMBOLS * MS + at]
                cosines[f] = c if cosines[f] is None else cosines[f] + c
                sines[f] = n if sines[f] is None else sines[f] + n
    lane16 = lax.broadcasted_iota(jnp.int32, (SUB, LANES), 1)
    for f in range(MS):
        turned = pltpu.roll(sines[f], 64, 1)
        value = cosines[f] + jnp.where(lane16 < 64, turned, -turned)
        out_ref[0, f, :, :] = value[:, 0:64]
        out_ref[1, f, :, :] = pltpu.roll(value, 64, 1)[:, 0:64]

    index_copies.wait_send()
    copies.wait_send()


def body(samples, constellation_index, pilot_offsets, cp_offset):
    consts = [jnp.asarray(table) for table in tables()]
    vmem = pl.BlockSpec(memory_space=pltpu.VMEM)
    hbm = pl.BlockSpec(memory_space=pl.ANY)
    records = samples.reshape(2 * MS * RECORD, LANES)
    doppler = consts[-1]
    out = pl.pallas_call(
        kernel,
        out_shape=pltpu.VMEM((2, MS, SUB, GUARD // SUB), F32),
        in_specs=[hbm] * (4 + len(consts)),
        out_specs=vmem,
        scratch_shapes=[
            pltpu.SMEM((MS,), jnp.int32),
            pltpu.SMEM((MS,), jnp.int32),
            pltpu.VMEM(records.shape, F32),
            pltpu.VMEM(constellation_index.shape, jnp.int32),
            *[pltpu.VMEM(table.shape, table.dtype) for table in consts[:-1]],
            pltpu.SMEM((1, doppler.shape[1]), F32),
            pltpu.VMEM((RADIX * MS, 512), BF16),
            pltpu.VMEM((RADIX * MS, 512), BF16),
            pltpu.VMEM((2 * MS, LANES), BF16),
            pltpu.VMEM((SUB, 2 * MS, LANES), BF16),
            pltpu.VMEM((16 * SUB, LANES), F32),
            pltpu.VMEM((2, 64, LANES), jnp.int32),
            pltpu.VMEM((SUB, 8, LANES), jnp.int16),
            pltpu.VMEM((SYM * SUB, 8, LANES), jnp.int16),
            pltpu.VMEM((8 * SYM * SUB, LANES), F32),
            pltpu.SemaphoreType.DMA((13,)),
            pltpu.SemaphoreType.DMA,
            pltpu.SemaphoreType.DMA,
            pltpu.SemaphoreType.DMA,
            pltpu.SemaphoreType.DMA,
            pltpu.SemaphoreType.REGULAR,
            pltpu.SemaphoreType.REGULAR,
        ],
        compiler_params=pltpu.CompilerParams(collective_id=0, has_side_effects=True),
    )(cp_offset, pilot_offsets, records, constellation_index, *consts)
    return out.transpose(0, 2, 1, 3)


def solution(mesh):
    return jax.shard_map(
        body,
        mesh=mesh,
        in_specs=(
            P(None, ("chan", "sub"), "sym", None),
            P(("chan", "sym"), "sub"),
            P("sym"),
            P(("chan", "sym")),
        ),
        out_specs=P(None, "chan", "sym", "sub"),
        check_vma=False,
    )
```

```python
import functools
import math

import jax
import jax.numpy as jnp
import ml_dtypes
import numpy as np
from jax import lax
from jax.experimental import pallas as pl
from jax.experimental.pallas import tpu as pltpu
from jax.sharding import PartitionSpec as P

MESH = pl.DeviceIdType.MESH
BF16 = jnp.bfloat16
F32 = jnp.float32

LENGTH = 8192
TONES = 4096
LOWEST = 2048
RADIX = 32
LANES = 128
GUARD = 1024
HALFSPAN = 48
PSP = 12
SYM = 4
SUB = 16
MS = 6
SYMBOLS = 24
SHIFTS = (-2, -1, 0, 1, 2)
FAR_FIRST = (10, 11, 8, 9, 6, 7, 14, 15, 4, 5, 12, 13, 2, 3, 1)


def halves(matrix):
    high = matrix.astype(ml_dtypes.bfloat16)
    low = (matrix - high.astype(np.float64)).astype(ml_dtypes.bfloat16)
    return high, low


def tables():
    p = np.arange(RADIX)
    turn = 2.0 * np.pi
    c = np.cos(turn * np.outer(p, p) / RADIX)
    s = np.sin(turn * np.outer(p, p) / RADIX)
    high, low = halves(np.block([[c, s], [-s, c]]))
    first = np.concatenate([high, low, high], axis=1)
    b = np.arange(256)
    angle = turn * np.outer(p, b) / LENGTH
    twist = np.stack([np.cos(angle), np.sin(angle)]).astype(np.float32)
    j = LOWEST // RADIX + np.arange(LANES)
    angle = turn * (np.outer(b, j) % 256) / 256
    c, s = np.cos(angle), np.sin(angle)
    second = np.stack(halves(np.block([[c, -s], [s, c]]) / math.sqrt(LENGTH)))
    rows = []
    for shift in SHIFTS:
        gap = RADIX * shift + p[None, :] - p[:, None]
        rows.append(np.maximum(HALFSPAN + 1 - np.abs(gap), 0))
    taper = np.concatenate(rows, axis=0)
    taper = np.concatenate([taper, taper], axis=1).astype(ml_dtypes.bfloat16)
    v = np.arange(LANES)
    angle = turn * (np.outer(v, v) % LANES) / LANES
    c, s = np.cos(angle), np.sin(angle)
    third = np.stack(halves(np.block([[c, s], [-s, c]]) / math.sqrt(TONES * SYMBOLS)))
    angle = turn * np.outer(p, v) / TONES
    twirl = np.stack([np.cos(angle), np.sin(angle)]).astype(np.float32)
    u = np.arange(GUARD // LANES)
    angle = turn * (np.outer(u, p) % RADIX) / RADIX
    c, s = np.cos(angle), np.sin(angle)
    high, low = halves(np.block([[c, -s], [s, c]]))
    fourth = np.concatenate([high, low, high], axis=1)
    spread = np.zeros((4, RADIX, LANES), ml_dtypes.bfloat16)
    for g in range(4):
        for half in range(2):
            for owner in range(SUB):
                spread[g, SUB * half + owner, 4 * (2 * owner + half) + g] = 1
    f, m = np.arange(MS), np.arange(SYMBOLS)
    doppler = np.zeros((SYM, 2, MS, SYMBOLS), np.float32)
    for block in range(SYM):
        angle = turn * (np.outer(MS * block + f, m) % SYMBOLS) / SYMBOLS
        doppler[block] = np.cos(angle), np.sin(angle)
    doppler = doppler.reshape(SYM, 2 * MS * SYMBOLS)
    return first, twist, second, taper, third, twirl, fourth, spread, doppler


def dot(a, b):
    return jnp.dot(a, b, preferred_element_type=F32)


def parted(value):
    high = value.astype(BF16)
    low = (value - high.astype(F32)).astype(BF16)
    return high, low


RECORD = 72


def kernel(
    cp_hbm,
    pilot_hbm,
    x_hbm,
    index_hbm,
    first_hbm,
    twist_hbm,
    second_hbm,
    taper_hbm,
    third_hbm,
    twirl_hbm,
    fourth_hbm,
    spread_hbm,
    doppler_hbm,
    out_ref,
    cp_ref,
    pilot_ref,
    x_ref,
    index_ref,
    first_ref,
    twist_ref,
    second_ref,
    taper_ref,
    third_ref,
    twirl_ref,
    fourth_ref,
    spread_ref,
    doppler_ref,
    zh_ref,
    zl_ref,
    isend_ref,
    igath_ref,
    ig_ref,
    stage_ref,
    send_ref,
    recv_ref,
    got_ref,
    load_sem,
    isend_sem,
    irecv_sem,
    send_sem,
    recv_sem,
    near_sem,
    far_sem,
):
    sym = lax.axis_index("sym")
    sub = lax.axis_index("sub")
    barrier = pltpu.get_barrier_semaphore()
    before, after = lax.rem(sym + SYM - 1, SYM), lax.rem(sym + 1, SYM)

    for d in FAR_FIRST:
        pl.semaphore_signal(
            barrier, inc=1, device_id={"sub": lax.rem(sub + d, SUB)}, device_id_type=MESH
        )
    for to in (before, after):
        pl.semaphore_signal(barrier, inc=1, device_id={"sym": to}, device_id_type=MESH)

    loads = [
        pltpu.make_async_copy(source, target, load_sem.at[i])
        for i, (source, target) in enumerate(
            (
                (index_hbm, index_ref),
                (cp_hbm, cp_ref),
                (x_hbm, x_ref),
                (first_hbm, first_ref),
                (twist_hbm, twist_ref),
                (second_hbm, second_ref),
                (pilot_hbm, pilot_ref),
                (spread_hbm, spread_ref),
                (taper_hbm, taper_ref),
                (third_hbm, third_ref),
                (twirl_hbm, twirl_ref),
                (fourth_hbm, fourth_ref),
                (doppler_hbm.at[pl.ds(sym, 1)], doppler_ref),
            )
        )
    ]
    for load in loads:
        load.start()

    lane = lax.broadcasted_iota(jnp.int32, (RADIX, LANES), 1)
    row = lax.broadcasted_iota(jnp.int32, (RADIX, LANES), 0)
    row8 = lax.broadcasted_iota(jnp.int32, (8, LANES), 0)
    lane8 = lax.broadcasted_iota(jnp.int32, (8, LANES), 1)
    residue = lax.rem(RADIX * lane + row, PSP)

    loads[0].wait()
    index = index_ref[...].astype(F32)
    isend_ref[...] = jnp.concatenate([index[:, :LANES], index[:, LANES:]], axis=0).astype(BF16)

    pl.semaphore_wait(barrier, SUB + 1)
    for d in FAR_FIRST:
        pltpu.make_async_remote_copy(
            src_ref=isend_ref,
            dst_ref=igath_ref.at[sub],
            send_sem=isend_sem,
            recv_sem=irecv_sem,
            device_id={"sub": lax.rem(sub + d, SUB)},
            device_id_type=MESH,
        ).start()
    for to in (before, after):
        pl.semaphore_signal(near_sem, inc=1, device_id={"sym": to}, device_id_type=MESH)
    igath_ref[sub] = isend_ref[...]

    loads[1].wait()
    start_lanes = jnp.zeros((RADIX, LANES), jnp.int32)
    start_rows = jnp.zeros((8, LANES), jnp.int32)
    for m in range(MS):
        start_lanes = jnp.where(lane == m, cp_ref[m], start_lanes)
        start_rows = jnp.where(row8 == m, cp_ref[m], start_rows)
    step = 2.0 * math.pi / LENGTH
    angle = ((start_lanes * row) & (LENGTH - 1)).astype(F32) * step
    row_cos, row_sin = jnp.cos(angle), jnp.sin(angle)
    angle = ((start_rows * (LOWEST + RADIX * lane8)) & (LENGTH - 1)).astype(F32) * step
    lane_cos, lane_sin = jnp.cos(angle), jnp.sin(angle)

    for i in (2, 3, 4):
        loads[i].wait()
    place = LANES * row8 + lane8
    twist_cos, twist_sin = twist_ref[0], twist_ref[1]
    for m in range(MS):
        pieces = []
        for part in range(2):
            base = RECORD * (MS * part + m)
            x_ref[pl.ds(base, 8), :] = jnp.where(
                place >= cp_ref[m], x_ref[pl.ds(base, 8), :], x_ref[pl.ds(base + 64, 8), :]
            )
            pieces.append(
                jnp.concatenate(
                    [x_ref[pl.ds(base + i, RADIX, stride=2), :] for i in range(2)], axis=1
                )
            )
        high, low = parted(jnp.concatenate(pieces, axis=0))
        y = dot(first_ref[...], jnp.concatenate([high, high, low], axis=0))
        re, im = y[:RADIX], y[RADIX:]
        z = jnp.concatenate(
            [re * twist_cos + im * twist_sin, im * twist_cos - re * twist_sin], axis=1
        )
        high, low = parted(z)
        zh_ref[pl.ds(RADIX * m, RADIX), :] = high
        zl_ref[pl.ds(RADIX * m, RADIX), :] = low
    loads[5].wait()
    zh = zh_ref[...]
    spectra = dot(zh, second_ref[0]) + dot(zl_ref[...], second_ref[0]) + dot(zh, second_ref[1])


    for i in range(6, 13):
        loads[i].wait()

    def tapering(right, part):
        tapered = dot(taper_ref[:, : right.shape[0]], right)
        sums = []
        for i in range(part):
            total = None
            for at, shift in enumerate(SHIFTS):
                term = tapered[RADIX * at : RADIX * (at + 1), LANES * i : LANES * (i + 1)]
                if shift:
                    term = pltpu.roll(term, (-shift) % LANES, 1)
                    inside = lane < LANES - shift if shift > 0 else lane >= -shift
                    term = jnp.where(inside, term, 0.0)
                total = term if total is None else total + term
            sums.append(total)
        return sums

    turned = []
    pilots = []
    for m in range(MS):
        rows = slice(RADIX * m, RADIX * (m + 1))
        lc = lane_cos[m : m + 1, :]
        ls = lane_sin[m : m + 1, :]
        rc = jnp.broadcast_to(row_cos[:, m : m + 1], (RADIX, LANES))
        rs = jnp.broadcast_to(row_sin[:, m : m + 1], (RADIX, LANES))
        phase_re = lc * rc - ls * rs
        phase_im = lc * rs + ls * rc
        re, im = spectra[rows, :LANES], spectra[rows, LANES:]
        turned.append((re * phase_re - im * phase_im, re * phase_im + im * phase_re))
        pilots.append(residue == pilot_ref[m])
    inverses = []
    for m in range(0, MS, 2):
        right = jnp.concatenate([pilots[m].astype(BF16), pilots[m + 1].astype(BF16)], axis=1)
        inverses += [1.0 / total for total in tapering(right, 2)]
    pl.semaphore_wait(near_sem, 2)
    pl.semaphore_signal(far_sem, inc=1, device_id={"sym": before}, device_id_type=MESH)

    all_index = igath_ref.at[pl.ds(0, SUB - 1)]
    index_copies = pltpu.make_async_remote_copy(
        src_ref=all_index,
        dst_ref=all_index,
        send_sem=isend_sem,
        recv_sem=irecv_sem,
        device_id={"sub": lax.rem(sub + 1, SUB)},
        device_id_type=MESH,
    )
    index_copies.wait_recv()
    for owner in range(SUB):
        ig_ref[pl.ds(16 * owner, 2 * MS), :] = igath_ref[owner].astype(F32)

    natural = []
    for m in range(MS):
        value = jnp.concatenate(
            [ig_ref[pl.ds(MS * half + m, SUB, stride=16), :] for half in range(2)], axis=0
        )
        natural.append(jnp.transpose(value).astype(BF16))
    index = sum(
        dot(
            jnp.concatenate([value[RADIX * g : RADIX * (g + 1)] for value in natural], axis=0),
            spread_ref[g],
        )
        for g in range(4)
    )

    high_rows, low_rows = [], []
    for m in range(MS):
        rows = slice(RADIX * m, RADIX * (m + 1))
        quadrature = jnp.floor(index[rows] * 0.125)
        level_re = 2.0 * (index[rows] - 8.0 * quadrature) - 7.0
        level_im = 2.0 * quadrature - 7.0
        factor = math.sqrt(42.0) / (level_re * level_re + level_im * level_im)
        scaled_re, scaled_im = level_re * factor, level_im * factor
        re, im = turned[m]
        ratio_re = re * scaled_re + im * scaled_im
        ratio_im = im * scaled_re - re * scaled_im
        picked = jnp.concatenate(
            [jnp.where(pilots[m], ratio_re, 0.0), jnp.where(pilots[m], ratio_im, 0.0)], axis=1
        )
        high, low = parted(picked)
        sums = tapering(jnp.concatenate([high, low], axis=0), 2)
        cleaned = jnp.concatenate(
            [ratio_re - sums[0] * inverses[m], ratio_im - sums[1] * inverses[m]], axis=1
        )
        high, low = parted(cleaned)
        high_rows.append(high)
        low_rows.append(low)
    high = jnp.concatenate(high_rows, axis=0)
    low = jnp.concatenate(low_rows, axis=0)
    folded = dot(high, third_ref[0]) + dot(low, third_ref[0]) + dot(high, third_ref[1])

    twirl_cos, twirl_sin = twirl_ref[0], twirl_ref[1]
    columns = []
    for m in range(MS):
        rows = slice(RADIX * m, RADIX * (m + 1))
        re, im = folded[rows, :LANES], folded[rows, LANES:]
        value = jnp.concatenate(
            [re * twirl_cos - im * twirl_sin, re * twirl_sin + im * twirl_cos], axis=0
        )
        high, low = parted(value)
        columns.append(jnp.concatenate([high, high, low], axis=0))
    profile = dot(fourth_ref[...], jnp.concatenate(columns, axis=1))

    pairs = []
    for m in range(MS):
        re = profile[0:8, LANES * m : LANES * (m + 1)]
        im = profile[8:16, LANES * m : LANES * (m + 1)]
        pairs.append(
            (
                jnp.where(lane8 < 64, re, pltpu.roll(im, 64, 1)),
                jnp.where(lane8 < 64, pltpu.roll(re, 64, 1), im),
            )
        )
    for half in range(2):
        largest = functools.reduce(jnp.maximum, [jnp.abs(pair[half]) for pair in pairs])
        largest = jnp.maximum(jnp.max(largest, axis=1, keepdims=True), 1e-30)
        code = jnp.broadcast_to(jnp.ceil(jnp.log2(largest) * 256.0), (8, LANES))
        inverse = 32767.0 * jnp.exp2(code * (-1.0 / 256.0))
        for m in range(MS):
            value = jnp.clip(jnp.round(pairs[m][half] * inverse), -32767.0, 32767.0)
            stage_ref[half, pl.ds(m, 8, stride=8), :] = value.astype(jnp.int32)
        stage_ref[half, pl.ds(MS, 8, stride=8), :] = code.astype(jnp.int32)
        stage_ref[half, pl.ds(MS + 1, 8, stride=8), :] = jnp.zeros((8, LANES), jnp.int32)
        for u in range(8):
            send_ref[2 * u + half] = stage_ref[half, pl.ds(8 * u, 8), :].astype(jnp.int16)

    pl.semaphore_wait(far_sem, 1)
    slot = SUB * sym + sub
    for e in (2, 1, 3, 0):
        for d in (8, 9, 10, 11, 4, 5, 6, 7, 12, 13, 14, 15, 2, 3, 1, 0):
            if e == 0 and d == 0:
                continue
            to_sub = lax.rem(sub + d, SUB)
            pltpu.make_async_remote_copy(
                src_ref=send_ref.at[to_sub],
                dst_ref=recv_ref.at[slot],
                send_sem=send_sem,
                recv_sem=recv_sem.at[e],
                device_id={"sym": lax.rem(sym + e, SYM), "sub": to_sub},
                device_id_type=MESH,
            ).start()
    recv_ref[slot] = send_ref[sub]

    cosines = [None] * MS
    sines = [None] * MS
    for e in (0, 1, 3, 2):
        count = SUB - 1 if e == 0 else SUB
        some = recv_ref.at[pl.ds(0, count)]
        pltpu.make_async_remote_copy(
            src_ref=some,
            dst_ref=some,
            send_sem=send_sem,
            recv_sem=recv_sem.at[e],
            device_id={"sub": lax.rem(sub + 1, SUB)},
            device_id_type=MESH,
        ).wait_recv()
        source = lax.rem(sym + SYM - e, SYM)
        base = 8 * SUB * e
        for i in range(SUB):
            got_ref[pl.ds(base + 8 * i, 8), :] = (
                recv_ref[SUB * source + i].astype(jnp.int32).astype(F32)
            )
        code = got_ref[pl.ds(base + MS, SUB, stride=8), :]
        scale = jnp.exp2(code * (1.0 / 256.0)) * (1.0 / 32767.0)
        for m in range(MS):
            value = got_ref[pl.ds(base + m, SUB, stride=8), :] * scale
            for f in range(MS):
                at = SYMBOLS * f + MS * source + m
                c = value * doppler_ref[0, at]
                n = value * doppler_ref[0, SYMBOLS * MS + at]
                cosines[f] = c if cosines[f] is None else cosines[f] + c
                sines[f] = n if sines[f] is None else sines[f] + n
    lane16 = lax.broadcasted_iota(jnp.int32, (SUB, LANES), 1)
    for f in range(MS):
        turned = pltpu.roll(sines[f], 64, 1)
        value = cosines[f] + jnp.where(lane16 < 64, turned, -turned)
        out_ref[0, f, :, :] = value[:, 0:64]
        out_ref[1, f, :, :] = pltpu.roll(value, 64, 1)[:, 0:64]

    index_copies.wait_send()
    everything = recv_ref.at[pl.ds(0, SYM * SUB - 1)]
    pltpu.make_async_remote_copy(
        src_ref=everything,
        dst_ref=everything,
        send_sem=send_sem,
        recv_sem=recv_sem.at[0],
        device_id={"sub": lax.rem(sub + 1, SUB)},
        device_id_type=MESH,
    ).wait_send()


def body(samples, constellation_index, pilot_offsets, cp_offset):
    consts = [jnp.asarray(table) for table in tables()]
    vmem = pl.BlockSpec(memory_space=pltpu.VMEM)
    hbm = pl.BlockSpec(memory_space=pl.ANY)
    records = samples.reshape(2 * MS * RECORD, LANES)
    doppler = consts[-1]
    out = pl.pallas_call(
        kernel,
        out_shape=pltpu.VMEM((2, MS, SUB, GUARD // SUB), F32),
        in_specs=[hbm] * (4 + len(consts)),
        out_specs=vmem,
        scratch_shapes=[
            pltpu.SMEM((MS,), jnp.int32),
            pltpu.SMEM((MS,), jnp.int32),
            pltpu.VMEM(records.shape, F32),
            pltpu.VMEM(constellation_index.shape, jnp.int32),
            *[pltpu.VMEM(table.shape, table.dtype) for table in consts[:-1]],
            pltpu.SMEM((1, doppler.shape[1]), F32),
            pltpu.VMEM((RADIX * MS, 512), BF16),
            pltpu.VMEM((RADIX * MS, 512), BF16),
            pltpu.VMEM((2 * MS, LANES), BF16),
            pltpu.VMEM((SUB, 2 * MS, LANES), BF16),
            pltpu.VMEM((16 * SUB, LANES), F32),
            pltpu.VMEM((2, 64, LANES), jnp.int32),
            pltpu.VMEM((SUB, 8, LANES), jnp.int16),
            pltpu.VMEM((SYM * SUB, 8, LANES), jnp.int16),
            pltpu.VMEM((8 * SYM * SUB, LANES), F32),
            pltpu.SemaphoreType.DMA((13,)),
            pltpu.SemaphoreType.DMA,
            pltpu.SemaphoreType.DMA,
            pltpu.SemaphoreType.DMA,
            pltpu.SemaphoreType.DMA((SYM,)),
            pltpu.SemaphoreType.REGULAR,
            pltpu.SemaphoreType.REGULAR,
        ],
        compiler_params=pltpu.CompilerParams(collective_id=0, has_side_effects=True),
    )(cp_offset, pilot_offsets, records, constellation_index, *consts)
    return out.transpose(0, 2, 1, 3)


def solution(mesh):
    return jax.shard_map(
        body,
        mesh=mesh,
        in_specs=(
            P(None, ("chan", "sub"), "sym", None),
            P(("chan", "sym"), "sub"),
            P("sym"),
            P(("chan", "sym")),
        ),
        out_specs=P(None, "chan", "sym", "sub"),
        check_vma=False,
    )
```

```python
import functools
import math

import jax
import jax.numpy as jnp
import ml_dtypes
import numpy as np
from jax import lax
from jax.experimental import pallas as pl
from jax.experimental.pallas import tpu as pltpu
from jax.sharding import PartitionSpec as P

MESH = pl.DeviceIdType.MESH
BF16 = jnp.bfloat16
F32 = jnp.float32

LENGTH = 8192
TONES = 4096
LOWEST = 2048
RADIX = 32
LANES = 128
GUARD = 1024
HALFSPAN = 48
PSP = 12
SYM = 4
SUB = 16
MS = 6
HS = 3
SYMBOLS = 24
SHIFTS = ((0, 0, 32), (-1, 0, 32), (1, 0, 32), (-2, 0, 16), (2, 16, 32))
FAR_FIRST = (10, 11, 8, 9, 6, 7, 14, 15, 4, 5, 12, 13, 2, 3, 1)


def halves(matrix):
    high = matrix.astype(ml_dtypes.bfloat16)
    low = (matrix - high.astype(np.float64)).astype(ml_dtypes.bfloat16)
    return high, low


def tables():
    p = np.arange(RADIX)
    turn = 2.0 * np.pi
    c = np.cos(turn * np.outer(p, p) / RADIX)
    s = np.sin(turn * np.outer(p, p) / RADIX)
    high, low = halves(np.block([[c, s], [-s, c]]))
    first = np.concatenate([high, low, high], axis=1)
    b = np.arange(256)
    angle = turn * np.outer(p, b) / LENGTH
    twist = np.stack([np.cos(angle), np.sin(angle)]).astype(np.float32)
    j = LOWEST // RADIX + np.arange(LANES)
    angle = turn * (np.outer(b, j) % 256) / 256
    c, s = np.cos(angle), np.sin(angle)
    second = np.stack(halves(np.block([[c, -s], [s, c]]) / math.sqrt(LENGTH)))
    rows = []
    for shift, low, high in SHIFTS:
        gap = RADIX * shift + p[None, :] - p[low:high, None]
        rows.append(np.maximum(HALFSPAN + 1 - np.abs(gap), 0))
    taper = np.concatenate(rows, axis=0)
    taper = np.concatenate([taper, taper], axis=1).astype(ml_dtypes.bfloat16)
    v = np.arange(LANES)
    angle = turn * (np.outer(v, v) % LANES) / LANES
    c, s = np.cos(angle), np.sin(angle)
    third = np.stack(halves(np.block([[c, s], [-s, c]]) / math.sqrt(TONES * SYMBOLS)))
    angle = turn * np.outer(p, v) / TONES
    twirl = np.stack([np.cos(angle), np.sin(angle)]).astype(np.float32)
    u = np.arange(GUARD // LANES)
    angle = turn * (np.outer(u, p) % RADIX) / RADIX
    c, s = np.cos(angle), np.sin(angle)
    high, low = halves(np.block([[c, -s], [s, c]]))
    fourth = np.concatenate([high, low, high], axis=1)
    spread = np.zeros((4, RADIX, LANES), ml_dtypes.bfloat16)
    for g in range(4):
        for half in range(2):
            for owner in range(SUB):
                spread[g, SUB * half + owner, 4 * (2 * owner + half) + g] = 1
    f, m = np.arange(MS), np.arange(SYMBOLS)
    doppler = np.zeros((SYM, 2, MS, SYMBOLS), np.float32)
    for block in range(SYM):
        angle = turn * (np.outer(MS * block + f, m) % SYMBOLS) / SYMBOLS
        doppler[block] = np.cos(angle), np.sin(angle)
    doppler = doppler.reshape(SYM, 2 * MS * SYMBOLS)
    return first, twist, second, taper, third, twirl, fourth, spread, doppler


def dot(a, b):
    return jnp.dot(a, b, preferred_element_type=F32)


def parted(value):
    high = value.astype(BF16)
    low = (value - high.astype(F32)).astype(BF16)
    return high, low


RECORD = 72


def kernel(
    cp_hbm,
    pilot_hbm,
    x_hbm,
    index_hbm,
    first_hbm,
    twist_hbm,
    second_hbm,
    taper_hbm,
    third_hbm,
    twirl_hbm,
    fourth_hbm,
    spread_hbm,
    doppler_hbm,
    out_ref,
    cp_ref,
    pilot_ref,
    x_ref,
    index_ref,
    first_ref,
    twist_ref,
    second_ref,
    taper_ref,
    third_ref,
    twirl_ref,
    fourth_ref,
    spread_ref,
    doppler_ref,
    zh_ref,
    zl_ref,
    isend_ref,
    igath_ref,
    ig_ref,
    stage_ref,
    send_ref,
    recv_ref,
    got_ref,
    load_sem,
    swap_sem,
    isend_sem,
    irecv_sem,
    send_sem,
    recv_sem,
    near_sem,
    far_sem,
):
    sym = lax.axis_index("sym")
    sub = lax.axis_index("sub")
    barrier = pltpu.get_barrier_semaphore()
    before, after = lax.rem(sym + SYM - 1, SYM), lax.rem(sym + 1, SYM)
    core, pair = lax.rem(sub, 2), sub // 2
    other = 1 - core

    for d in FAR_FIRST:
        pl.semaphore_signal(
            barrier, inc=1, device_id={"sub": lax.rem(sub + d, SUB)}, device_id_type=MESH
        )
    for to in (before, after):
        pl.semaphore_signal(barrier, inc=1, device_id={"sym": to}, device_id_type=MESH)

    def records(part, taker):
        return pl.ds(pl.multiple_of(RECORD * (MS * part + HS * taker), 8), RECORD * HS)

    def places(channel, part):
        return pl.ds(pl.multiple_of(RECORD * HS * (2 * channel + part), 8), RECORD * HS)

    loads = [
        pltpu.make_async_copy(source, target, load_sem.at[i])
        for i, (source, target) in enumerate(
            (
                (index_hbm, index_ref),
                (cp_hbm, cp_ref),
                (first_hbm, first_ref),
                (twist_hbm, twist_ref),
                (second_hbm, second_ref),
                (pilot_hbm, pilot_ref),
                (spread_hbm, spread_ref),
                (taper_hbm, taper_ref),
                (third_hbm, third_ref),
                (twirl_hbm, twirl_ref),
                (fourth_hbm, fourth_ref),
                (doppler_hbm.at[pl.ds(sym, 1)], doppler_ref),
            )
        )
    ]
    for part in range(2):
        loads.append(
            pltpu.make_async_copy(
                x_hbm.at[records(part, core)], x_ref.at[places(core, part)], load_sem.at[12 + part]
            )
        )
    for load in loads:
        load.start()

    lane = lax.broadcasted_iota(jnp.int32, (RADIX, LANES), 1)
    row = lax.broadcasted_iota(jnp.int32, (RADIX, LANES), 0)
    row8 = lax.broadcasted_iota(jnp.int32, (8, LANES), 0)
    lane8 = lax.broadcasted_iota(jnp.int32, (8, LANES), 1)
    residue = lax.rem(RADIX * lane + row, PSP)

    loads[0].wait()
    index = index_ref[...].astype(F32)
    for taker in range(2):
        rows = slice(HS * taker, HS * (taker + 1))
        isend_ref[taker] = jnp.concatenate(
            [index[rows, :LANES], index[rows, LANES:]], axis=0
        ).astype(BF16)

    pl.semaphore_wait(barrier, SUB + 1)
    for d in FAR_FIRST:
        pltpu.make_async_remote_copy(
            src_ref=isend_ref.at[lax.rem(sub + d, 2)],
            dst_ref=igath_ref.at[sub],
            send_sem=isend_sem,
            recv_sem=irecv_sem,
            device_id={"sub": lax.rem(sub + d, SUB)},
            device_id_type=MESH,
        ).start()
    for to in (before, after):
        pl.semaphore_signal(near_sem, inc=1, device_id={"sym": to}, device_id_type=MESH)
    igath_ref[sub] = isend_ref[core]
    swaps = []
    for part in range(2):
        swaps.append(
            pltpu.make_async_remote_copy(
                src_ref=x_hbm.at[records(part, other)],
                dst_ref=x_ref.at[places(core, part)],
                send_sem=swap_sem.at[part],
                recv_sem=swap_sem.at[2 + part],
                device_id={"sub": sub + 1 - 2 * core},
                device_id_type=MESH,
            )
        )
        swaps[part].start()

    loads[1].wait()
    start_lanes = jnp.zeros((RADIX, LANES), jnp.int32)
    start_rows = jnp.zeros((8, LANES), jnp.int32)
    starts = [cp_ref[HS * core + i] for i in range(HS)]
    for i in range(HS):
        start_lanes = jnp.where(lane == i, starts[i], start_lanes)
        start_rows = jnp.where(row8 == i, starts[i], start_rows)
    step = 2.0 * math.pi / LENGTH
    angle = ((start_lanes * row) & (LENGTH - 1)).astype(F32) * step
    row_cos, row_sin = jnp.cos(angle), jnp.sin(angle)
    angle = ((start_rows * (LOWEST + RADIX * lane8)) & (LENGTH - 1)).astype(F32) * step
    lane_cos, lane_sin = jnp.cos(angle), jnp.sin(angle)

    for i in (2, 3, 12, 13):
        loads[i].wait()
    place = LANES * row8 + lane8
    twist_cos, twist_sin = twist_ref[0], twist_ref[1]
    for turn, channel in enumerate((core, other)):
        if turn:
            for swap in swaps:
                swap.wait_recv()
        for i in range(HS):
            pieces = []
            for part in range(2):
                base = pl.multiple_of(RECORD * (HS * (2 * channel + part) + i), 8)
                x_ref[pl.ds(base, 8), :] = jnp.where(
                    place >= starts[i], x_ref[pl.ds(base, 8), :], x_ref[pl.ds(base + 64, 8), :]
                )
                pieces.append(
                    jnp.concatenate(
                        [x_ref[pl.ds(base + n, RADIX, stride=2), :] for n in range(2)], axis=1
                    )
                )
            high, low = parted(jnp.concatenate(pieces, axis=0))
            y = dot(first_ref[...], jnp.concatenate([high, high, low], axis=0))
            re, im = y[:RADIX], y[RADIX:]
            z = jnp.concatenate(
                [re * twist_cos + im * twist_sin, im * twist_cos - re * twist_sin], axis=1
            )
            high, low = parted(z)
            rows = pl.ds(pl.multiple_of(RADIX * (HS * channel + i), RADIX), RADIX)
            zh_ref[rows, :] = high
            zl_ref[rows, :] = low
    loads[4].wait()
    zh = zh_ref[...]
    spectra = dot(zh, second_ref[0]) + dot(zl_ref[...], second_ref[0]) + dot(zh, second_ref[1])


    for i in range(5, 12):
        loads[i].wait()

    def tapering(right, count):
        tapered = dot(taper_ref[:, : right.shape[0]], right)
        sums = []
        for n in range(count):
            halves_of = [None, None]
            at = 0
            for shift, low, high in SHIFTS:
                term = tapered[at : at + high - low, LANES * n : LANES * (n + 1)]
                at += high - low
                if shift:
                    term = pltpu.roll(term, (-shift) % LANES, 1)
                    inside = lane[low:high] < LANES - shift if shift > 0 else lane[low:high] >= -shift
                    term = jnp.where(inside, term, 0.0)
                for half in range(2):
                    if low <= 16 * half < high:
                        piece = term[16 * half - low : 16 * half - low + 16]
                        halves_of[half] = (
                            piece if halves_of[half] is None else halves_of[half] + piece
                        )
            sums.append(jnp.concatenate(halves_of, axis=0))
        return sums

    turned = [None] * MS
    pilots = []
    for i in range(HS):
        lc = lane_cos[i : i + 1, :]
        ls = lane_sin[i : i + 1, :]
        rc = jnp.broadcast_to(row_cos[:, i : i + 1], (RADIX, LANES))
        rs = jnp.broadcast_to(row_sin[:, i : i + 1], (RADIX, LANES))
        phase_re = lc * rc - ls * rs
        phase_im = lc * rs + ls * rc
        for channel in range(2):
            m = HS * channel + i
            rows = slice(RADIX * m, RADIX * (m + 1))
            re, im = spectra[rows, :LANES], spectra[rows, LANES:]
            turned[m] = (re * phase_re - im * phase_im, re * phase_im + im * phase_re)
        pilots.append(residue == pilot_ref[HS * core + i])
    right = jnp.concatenate([pilot.astype(BF16) for pilot in pilots], axis=1)
    inverses = [1.0 / total for total in tapering(right, HS)]
    pl.semaphore_wait(near_sem, 2)
    pl.semaphore_signal(far_sem, inc=1, device_id={"sym": before}, device_id_type=MESH)

    all_index = igath_ref.at[pl.ds(0, SUB - 1)]
    index_copies = pltpu.make_async_remote_copy(
        src_ref=all_index,
        dst_ref=all_index,
        send_sem=isend_sem,
        recv_sem=irecv_sem,
        device_id={"sub": lax.rem(sub + 1, SUB)},
        device_id_type=MESH,
    )
    index_copies.wait_recv()
    for owner in range(SUB):
        ig_ref[pl.ds(8 * owner, 2 * HS), :] = igath_ref[owner].astype(F32)

    natural = []
    for i in range(HS):
        value = jnp.concatenate(
            [ig_ref[pl.ds(HS * half + i, SUB, stride=8), :] for half in range(2)], axis=0
        )
        natural.append(jnp.transpose(value).astype(BF16))
    index = sum(
        dot(
            jnp.concatenate([value[RADIX * g : RADIX * (g + 1)] for value in natural], axis=0),
            spread_ref[g],
        )
        for g in range(4)
    )

    high_rows, low_rows = [None] * MS, [None] * MS
    for i in range(HS):
        value = index[RADIX * i : RADIX * (i + 1)]
        quadrature = jnp.floor(value * 0.125)
        level_re = 2.0 * (value - 8.0 * quadrature) - 7.0
        level_im = 2.0 * quadrature - 7.0
        factor = math.sqrt(42.0) / (level_re * level_re + level_im * level_im)
        scaled_re, scaled_im = level_re * factor, level_im * factor
        for m in (i, HS + i):
            re, im = turned[m]
            ratio_re = re * scaled_re + im * scaled_im
            ratio_im = im * scaled_re - re * scaled_im
            picked = jnp.concatenate(
                [jnp.where(pilots[i], ratio_re, 0.0), jnp.where(pilots[i], ratio_im, 0.0)], axis=1
            )
            high, low = parted(picked)
            sums = tapering(jnp.concatenate([high, low], axis=0), 2)
            cleaned = jnp.concatenate(
                [ratio_re - sums[0] * inverses[i], ratio_im - sums[1] * inverses[i]], axis=1
            )
            high_rows[m], low_rows[m] = parted(cleaned)
    high = jnp.concatenate(high_rows, axis=0)
    low = jnp.concatenate(low_rows, axis=0)
    folded = dot(high, third_ref[0]) + dot(low, third_ref[0]) + dot(high, third_ref[1])

    twirl_cos, twirl_sin = twirl_ref[0], twirl_ref[1]
    columns = []
    for m in range(MS):
        rows = slice(RADIX * m, RADIX * (m + 1))
        re, im = folded[rows, :LANES], folded[rows, LANES:]
        value = jnp.concatenate(
            [re * twirl_cos - im * twirl_sin, re * twirl_sin + im * twirl_cos], axis=0
        )
        high, low = parted(value)
        columns.append(jnp.concatenate([high, high, low], axis=0))
    profile = dot(fourth_ref[...], jnp.concatenate(columns, axis=1))

    pairs = []
    for m in range(MS):
        re = profile[0:8, LANES * m : LANES * (m + 1)]
        im = profile[8:16, LANES * m : LANES * (m + 1)]
        pairs.append(
            (
                jnp.where(lane8 < 64, re, pltpu.roll(im, 64, 1)),
                jnp.where(lane8 < 64, pltpu.roll(re, 64, 1), im),
            )
        )
    for half in range(2):
        for channel in range(2):
            some = [pairs[HS * channel + i][half] for i in range(HS)]
            largest = functools.reduce(jnp.maximum, [jnp.abs(value) for value in some])
            largest = jnp.maximum(jnp.max(largest, axis=1, keepdims=True), 1e-30)
            code = jnp.broadcast_to(jnp.ceil(jnp.log2(largest) * 256.0), (8, LANES))
            inverse = 32767.0 * jnp.exp2(code * (-1.0 / 256.0))
            for i in range(HS):
                value = jnp.clip(jnp.round(some[i] * inverse), -32767.0, 32767.0)
                stage_ref[half, pl.ds(4 * channel + i, 8, stride=8), :] = value.astype(jnp.int32)
            stage_ref[half, pl.ds(4 * channel + HS, 8, stride=8), :] = code.astype(jnp.int32)
        for u in range(8):
            send_ref[2 * u + half] = stage_ref[half, pl.ds(8 * u, 8), :].astype(jnp.int16)

    pl.semaphore_wait(far_sem, 1)
    slot = SUB * sym + 8 * core + pair
    for e in (2, 1, 3, 0):
        for d in (8, 9, 10, 11, 4, 5, 6, 7, 12, 13, 14, 15, 2, 3, 1, 0):
            if e == 0 and d == 0:
                continue
            to_sub = lax.rem(sub + d, SUB)
            pltpu.make_async_remote_copy(
                src_ref=send_ref.at[to_sub],
                dst_ref=recv_ref.at[slot],
                send_sem=send_sem,
                recv_sem=recv_sem.at[e],
                device_id={"sym": lax.rem(sym + e, SYM), "sub": to_sub},
                device_id_type=MESH,
            ).start()
    recv_ref[slot] = send_ref[sub]

    cosines = [None] * MS
    sines = [None] * MS
    for e in (0, 1, 3, 2):
        count = SUB - 1 if e == 0 else SUB
        some = recv_ref.at[pl.ds(0, count)]
        pltpu.make_async_remote_copy(
            src_ref=some,
            dst_ref=some,
            send_sem=send_sem,
            recv_sem=recv_sem.at[e],
            device_id={"sub": lax.rem(sub + 1, SUB)},
            device_id_type=MESH,
        ).wait_recv()
        source = lax.rem(sym + SYM - e, SYM)
        base = 8 * SUB * e
        for i in range(SUB):
            got_ref[pl.ds(base + 8 * i, 8), :] = (
                recv_ref[SUB * source + i].astype(jnp.int32).astype(F32)
            )
        for taker in range(2):
            first = base + 64 * taker
            code = got_ref[pl.ds(first + HS, SUB, stride=4), :]
            scale = jnp.exp2(code * (1.0 / 256.0)) * (1.0 / 32767.0)
            for i in range(HS):
                value = got_ref[pl.ds(first + i, SUB, stride=4), :] * scale
                for f in range(MS):
                    at = SYMBOLS * f + MS * source + HS * taker + i
                    c = value * doppler_ref[0, at]
                    n = value * doppler_ref[0, SYMBOLS * MS + at]
                    cosines[f] = c if cosines[f] is None else cosines[f] + c
                    sines[f] = n if sines[f] is None else sines[f] + n
    lane16 = lax.broadcasted_iota(jnp.int32, (SUB, LANES), 1)
    for f in range(MS):
        turned = pltpu.roll(sines[f], 64, 1)
        value = cosines[f] + jnp.where(lane16 < 64, turned, -turned)
        out_ref[0, f, :, :] = value[:, 0:64]
        out_ref[1, f, :, :] = pltpu.roll(value, 64, 1)[:, 0:64]

    index_copies.wait_send()
    for swap in swaps:
        swap.wait_send()
    everything = recv_ref.at[pl.ds(0, SYM * SUB - 1)]
    pltpu.make_async_remote_copy(
        src_ref=everything,
        dst_ref=everything,
        send_sem=send_sem,
        recv_sem=recv_sem.at[0],
        device_id={"sub": lax.rem(sub + 1, SUB)},
        device_id_type=MESH,
    ).wait_send()


def body(samples, constellation_index, pilot_offsets, cp_offset):
    consts = [jnp.asarray(table) for table in tables()]
    vmem = pl.BlockSpec(memory_space=pltpu.VMEM)
    hbm = pl.BlockSpec(memory_space=pl.ANY)
    records = samples.reshape(2 * MS * RECORD, LANES)
    doppler = consts[-1]
    out = pl.pallas_call(
        kernel,
        out_shape=pltpu.VMEM((2, MS, SUB, GUARD // SUB), F32),
        in_specs=[hbm] * (4 + len(consts)),
        out_specs=vmem,
        scratch_shapes=[
            pltpu.SMEM((MS,), jnp.int32),
            pltpu.SMEM((MS,), jnp.int32),
            pltpu.VMEM((4 * HS * RECORD, LANES), F32),
            pltpu.VMEM(constellation_index.shape, jnp.int32),
            *[pltpu.VMEM(table.shape, table.dtype) for table in consts[:-1]],
            pltpu.SMEM((1, doppler.shape[1]), F32),
            pltpu.VMEM((RADIX * MS, 512), BF16),
            pltpu.VMEM((RADIX * MS, 512), BF16),
            pltpu.VMEM((2, 2 * HS, LANES), BF16),
            pltpu.VMEM((SUB, 2 * HS, LANES), BF16),
            pltpu.VMEM((8 * SUB, LANES), F32),
            pltpu.VMEM((2, 64, LANES), jnp.int32),
            pltpu.VMEM((SUB, 8, LANES), jnp.int16),
            pltpu.VMEM((SYM * SUB, 8, LANES), jnp.int16),
            pltpu.VMEM((8 * SYM * SUB, LANES), F32),
            pltpu.SemaphoreType.DMA((14,)),
            pltpu.SemaphoreType.DMA((4,)),
            pltpu.SemaphoreType.DMA,
            pltpu.SemaphoreType.DMA,
            pltpu.SemaphoreType.DMA,
            pltpu.SemaphoreType.DMA((SYM,)),
            pltpu.SemaphoreType.REGULAR,
            pltpu.SemaphoreType.REGULAR,
        ],
        compiler_params=pltpu.CompilerParams(collective_id=0, has_side_effects=True),
    )(cp_offset, pilot_offsets, records, constellation_index, *consts)
    return out.transpose(0, 2, 1, 3)


def solution(mesh):
    return jax.shard_map(
        body,
        mesh=mesh,
        in_specs=(
            P(None, ("chan", "sub"), "sym", None),
            P(("chan", "sym"), "sub"),
            P("sym"),
            P(("chan", "sym")),
        ),
        out_specs=P(None, "chan", "sym", "sub"),
        check_vma=False,
    )
```

```python
import functools
import math

import jax
import jax.numpy as jnp
import ml_dtypes
import numpy as np
from jax import lax
from jax.experimental import pallas as pl
from jax.experimental.pallas import tpu as pltpu
from jax.sharding import PartitionSpec as P

MESH = pl.DeviceIdType.MESH
BF16 = jnp.bfloat16
F32 = jnp.float32

LENGTH = 8192
TONES = 4096
LOWEST = 2048
RADIX = 32
LANES = 128
GUARD = 1024
HALFSPAN = 48
PSP = 12
SYM = 4
SUB = 16
MS = 6
HS = 3
SYMBOLS = 24
SHIFTS = ((0, 0, 32), (-1, 0, 32), (1, 0, 32), (-2, 0, 16), (2, 16, 32))
STEPS = [(y, z, c) for y in range(4) for z in range(2) for c in range(2)]
FAR_FIRST = sorted(STEPS[1:], key=lambda step: -min(step[0], 4 - step[0]) - step[1] - 0.5 * step[2])


def hops(move):
    e, (y, z, c) = move
    along = 4 - z if e == 2 else 2 if e else z
    return min(y, 4 - y) + along + 0.5 * c


EXCHANGE = sorted(
    ((e, step) for e in range(SYM) for step in STEPS if e or any(step)), key=hops, reverse=True
)


def halves(matrix):
    high = matrix.astype(ml_dtypes.bfloat16)
    low = (matrix - high.astype(np.float64)).astype(ml_dtypes.bfloat16)
    return high, low


def tables():
    p = np.arange(RADIX)
    turn = 2.0 * np.pi
    c = np.cos(turn * np.outer(p, p) / RADIX)
    s = np.sin(turn * np.outer(p, p) / RADIX)
    high, low = halves(np.block([[c, s], [-s, c]]))
    first = np.concatenate([high, low, high], axis=1)
    b = np.arange(256)
    angle = turn * np.outer(p, b) / LENGTH
    twist = np.stack([np.cos(angle), np.sin(angle)]).astype(np.float32)
    j = LOWEST // RADIX + np.arange(LANES)
    angle = turn * (np.outer(b, j) % 256) / 256
    c, s = np.cos(angle), np.sin(angle)
    second = np.stack(halves(np.block([[c, -s], [s, c]]) / math.sqrt(LENGTH)))
    rows = []
    for shift, low, high in SHIFTS:
        gap = RADIX * shift + p[None, :] - p[low:high, None]
        rows.append(np.maximum(HALFSPAN + 1 - np.abs(gap), 0))
    taper = np.concatenate(rows, axis=0)
    taper = np.concatenate([taper, taper], axis=1).astype(ml_dtypes.bfloat16)
    v = np.arange(LANES)
    angle = turn * (np.outer(v, v) % LANES) / LANES
    c, s = np.cos(angle), np.sin(angle)
    third = np.stack(halves(np.block([[c, s], [-s, c]]) / math.sqrt(TONES * SYMBOLS)))
    angle = turn * np.outer(p, v) / TONES
    twirl = np.stack([np.cos(angle), np.sin(angle)]).astype(np.float32)
    u = np.arange(GUARD // LANES)
    angle = turn * (np.outer(u, p) % RADIX) / RADIX
    c, s = np.cos(angle), np.sin(angle)
    high, low = halves(np.block([[c, -s], [s, c]]))
    fourth = np.concatenate([high, low, high], axis=1)
    spread = np.zeros((4, RADIX, LANES), ml_dtypes.bfloat16)
    for g in range(4):
        for half in range(2):
            for owner in range(SUB):
                spread[g, SUB * half + owner, 4 * (2 * owner + half) + g] = 1
    f, m = np.arange(MS), np.arange(SYMBOLS)
    doppler = np.zeros((SYM, 2, MS, SYMBOLS), np.float32)
    for block in range(SYM):
        angle = turn * (np.outer(MS * block + f, m) % SYMBOLS) / SYMBOLS
        doppler[block] = np.cos(angle), np.sin(angle)
    doppler = doppler.reshape(SYM, 2 * MS * SYMBOLS)
    return first, twist, second, taper, third, twirl, fourth, spread, doppler


def dot(a, b):
    return jnp.dot(a, b, preferred_element_type=F32)


def parted(value):
    high = value.astype(BF16)
    low = (value - high.astype(F32)).astype(BF16)
    return high, low


RECORD = 72


def kernel(
    cp_hbm,
    pilot_hbm,
    x_hbm,
    index_hbm,
    first_hbm,
    twist_hbm,
    second_hbm,
    taper_hbm,
    third_hbm,
    twirl_hbm,
    fourth_hbm,
    spread_hbm,
    doppler_hbm,
    out_ref,
    cp_ref,
    pilot_ref,
    x_ref,
    index_ref,
    first_ref,
    twist_ref,
    second_ref,
    taper_ref,
    third_ref,
    twirl_ref,
    fourth_ref,
    spread_ref,
    doppler_ref,
    zh_ref,
    zl_ref,
    isend_ref,
    igath_ref,
    ig_ref,
    stage_ref,
    send_ref,
    recv_ref,
    got_ref,
    load_sem,
    swap_sem,
    isend_sem,
    irecv_sem,
    send_sem,
    recv_sem,
    near_sem,
    far_sem,
):
    sym = lax.axis_index("sym")
    sub = lax.axis_index("sub")
    barrier = pltpu.get_barrier_semaphore()
    before, after = lax.rem(sym + SYM - 1, SYM), lax.rem(sym + 1, SYM)
    core, pair = lax.rem(sub, 2), sub // 2
    other = 1 - core
    at_y = [4 * lax.rem(sub // 4 + y, 4) for y in range(4)]
    at_z = [2 * lax.rem(sub // 2 + z, 2) for z in range(2)]
    at_core = [core, other]

    def stepped(step):
        y, z, c = step
        return at_y[y] + at_z[z] + at_core[c]


    for step in FAR_FIRST:
        pl.semaphore_signal(
            barrier, inc=1, device_id={"sub": stepped(step)}, device_id_type=MESH
        )
    for to in (before, after):
        pl.semaphore_signal(barrier, inc=1, device_id={"sym": to}, device_id_type=MESH)

    def records(part, taker):
        return pl.ds(pl.multiple_of(RECORD * (MS * part + HS * taker), 8), RECORD * HS)

    def places(channel, part):
        return pl.ds(pl.multiple_of(RECORD * HS * (2 * channel + part), 8), RECORD * HS)

    loads = [
        pltpu.make_async_copy(source, target, load_sem.at[i])
        for i, (source, target) in enumerate(
            (
                (index_hbm, index_ref),
                (cp_hbm, cp_ref),
                (first_hbm, first_ref),
                (twist_hbm, twist_ref),
                (second_hbm, second_ref),
                (pilot_hbm, pilot_ref),
                (spread_hbm, spread_ref),
                (taper_hbm, taper_ref),
                (third_hbm, third_ref),
                (twirl_hbm, twirl_ref),
                (fourth_hbm, fourth_ref),
                (doppler_hbm.at[pl.ds(sym, 1)], doppler_ref),
            )
        )
    ]
    for part in range(2):
        loads.append(
            pltpu.make_async_copy(
                x_hbm.at[records(part, core)], x_ref.at[places(core, part)], load_sem.at[12 + part]
            )
        )
    for load in loads:
        load.start()

    lane = lax.broadcasted_iota(jnp.int32, (RADIX, LANES), 1)
    row = lax.broadcasted_iota(jnp.int32, (RADIX, LANES), 0)
    row8 = lax.broadcasted_iota(jnp.int32, (8, LANES), 0)
    lane8 = lax.broadcasted_iota(jnp.int32, (8, LANES), 1)
    residue = lax.rem(RADIX * lane + row, PSP)

    loads[0].wait()
    index = index_ref[...].astype(F32)
    for taker in range(2):
        rows = slice(HS * taker, HS * (taker + 1))
        isend_ref[taker] = jnp.concatenate(
            [index[rows, :LANES], index[rows, LANES:]], axis=0
        ).astype(BF16)

    pl.semaphore_wait(barrier, SUB + 1)
    for step in FAR_FIRST:
        pltpu.make_async_remote_copy(
            src_ref=isend_ref.at[at_core[step[2]]],
            dst_ref=igath_ref.at[sub],
            send_sem=isend_sem,
            recv_sem=irecv_sem,
            device_id={"sub": stepped(step)},
            device_id_type=MESH,
        ).start()
    for to in (before, after):
        pl.semaphore_signal(near_sem, inc=1, device_id={"sym": to}, device_id_type=MESH)
    igath_ref[sub] = isend_ref[core]
    swaps = []
    for part in range(2):
        swaps.append(
            pltpu.make_async_remote_copy(
                src_ref=x_hbm.at[records(part, other)],
                dst_ref=x_ref.at[places(core, part)],
                send_sem=swap_sem.at[part],
                recv_sem=swap_sem.at[2 + part],
                device_id={"sub": sub + 1 - 2 * core},
                device_id_type=MESH,
            )
        )
        swaps[part].start()

    loads[1].wait()
    start_lanes = jnp.zeros((RADIX, LANES), jnp.int32)
    start_rows = jnp.zeros((8, LANES), jnp.int32)
    starts = [cp_ref[HS * core + i] for i in range(HS)]
    for i in range(HS):
        start_lanes = jnp.where(lane == i, starts[i], start_lanes)
        start_rows = jnp.where(row8 == i, starts[i], start_rows)
    step = 2.0 * math.pi / LENGTH
    angle = ((start_lanes * row) & (LENGTH - 1)).astype(F32) * step
    row_cos, row_sin = jnp.cos(angle), jnp.sin(angle)
    angle = ((start_rows * (LOWEST + RADIX * lane8)) & (LENGTH - 1)).astype(F32) * step
    lane_cos, lane_sin = jnp.cos(angle), jnp.sin(angle)

    for i in (2, 3, 12, 13):
        loads[i].wait()
    place = LANES * row8 + lane8
    twist_cos, twist_sin = twist_ref[0], twist_ref[1]
    for turn, channel in enumerate((core, other)):
        if turn:
            for swap in swaps:
                swap.wait_recv()
        for i in range(HS):
            pieces = []
            for part in range(2):
                base = pl.multiple_of(RECORD * (HS * (2 * channel + part) + i), 8)
                x_ref[pl.ds(base, 8), :] = jnp.where(
                    place >= starts[i], x_ref[pl.ds(base, 8), :], x_ref[pl.ds(base + 64, 8), :]
                )
                pieces.append(
                    jnp.concatenate(
                        [x_ref[pl.ds(base + n, RADIX, stride=2), :] for n in range(2)], axis=1
                    )
                )
            high, low = parted(jnp.concatenate(pieces, axis=0))
            y = dot(first_ref[...], jnp.concatenate([high, high, low], axis=0))
            re, im = y[:RADIX], y[RADIX:]
            z = jnp.concatenate(
                [re * twist_cos + im * twist_sin, im * twist_cos - re * twist_sin], axis=1
            )
            high, low = parted(z)
            rows = pl.ds(pl.multiple_of(RADIX * (HS * channel + i), RADIX), RADIX)
            zh_ref[rows, :] = high
            zl_ref[rows, :] = low
    loads[4].wait()
    zh = zh_ref[...]
    spectra = dot(zh, second_ref[0]) + dot(zl_ref[...], second_ref[0]) + dot(zh, second_ref[1])


    for i in range(5, 12):
        loads[i].wait()

    def tapering(right, count):
        tapered = dot(taper_ref[:, : right.shape[0]], right)
        sums = []
        for n in range(count):
            halves_of = [None, None]
            at = 0
            for shift, low, high in SHIFTS:
                term = tapered[at : at + high - low, LANES * n : LANES * (n + 1)]
                at += high - low
                if shift:
                    term = pltpu.roll(term, (-shift) % LANES, 1)
                    inside = lane[low:high] < LANES - shift if shift > 0 else lane[low:high] >= -shift
                    term = jnp.where(inside, term, 0.0)
                for half in range(2):
                    if low <= 16 * half < high:
                        piece = term[16 * half - low : 16 * half - low + 16]
                        halves_of[half] = (
                            piece if halves_of[half] is None else halves_of[half] + piece
                        )
            sums.append(jnp.concatenate(halves_of, axis=0))
        return sums

    turned = [None] * MS
    pilots = []
    for i in range(HS):
        lc = lane_cos[i : i + 1, :]
        ls = lane_sin[i : i + 1, :]
        rc = jnp.broadcast_to(row_cos[:, i : i + 1], (RADIX, LANES))
        rs = jnp.broadcast_to(row_sin[:, i : i + 1], (RADIX, LANES))
        phase_re = lc * rc - ls * rs
        phase_im = lc * rs + ls * rc
        for channel in range(2):
            m = HS * channel + i
            rows = slice(RADIX * m, RADIX * (m + 1))
            re, im = spectra[rows, :LANES], spectra[rows, LANES:]
            turned[m] = (re * phase_re - im * phase_im, re * phase_im + im * phase_re)
        pilots.append(residue == pilot_ref[HS * core + i])
    right = jnp.concatenate([pilot.astype(BF16) for pilot in pilots], axis=1)
    inverses = [1.0 / total for total in tapering(right, HS)]
    pl.semaphore_wait(near_sem, 2)
    pl.semaphore_signal(far_sem, inc=1, device_id={"sym": before}, device_id_type=MESH)

    all_index = igath_ref.at[pl.ds(0, SUB - 1)]
    index_copies = pltpu.make_async_remote_copy(
        src_ref=all_index,
        dst_ref=all_index,
        send_sem=isend_sem,
        recv_sem=irecv_sem,
        device_id={"sub": lax.rem(sub + 1, SUB)},
        device_id_type=MESH,
    )
    index_copies.wait_recv()
    for owner in range(SUB):
        ig_ref[pl.ds(8 * owner, 2 * HS), :] = igath_ref[owner].astype(F32)

    natural = []
    for i in range(HS):
        value = jnp.concatenate(
            [ig_ref[pl.ds(HS * half + i, SUB, stride=8), :] for half in range(2)], axis=0
        )
        natural.append(jnp.transpose(value).astype(BF16))
    index = sum(
        dot(
            jnp.concatenate([value[RADIX * g : RADIX * (g + 1)] for value in natural], axis=0),
            spread_ref[g],
        )
        for g in range(4)
    )

    high_rows, low_rows = [None] * MS, [None] * MS
    for i in range(HS):
        value = index[RADIX * i : RADIX * (i + 1)]
        quadrature = jnp.floor(value * 0.125)
        level_re = 2.0 * (value - 8.0 * quadrature) - 7.0
        level_im = 2.0 * quadrature - 7.0
        factor = math.sqrt(42.0) / (level_re * level_re + level_im * level_im)
        scaled_re, scaled_im = level_re * factor, level_im * factor
        for m in (i, HS + i):
            re, im = turned[m]
            ratio_re = re * scaled_re + im * scaled_im
            ratio_im = im * scaled_re - re * scaled_im
            picked = jnp.concatenate(
                [jnp.where(pilots[i], ratio_re, 0.0), jnp.where(pilots[i], ratio_im, 0.0)], axis=1
            )
            high, low = parted(picked)
            sums = tapering(jnp.concatenate([high, low], axis=0), 2)
            cleaned = jnp.concatenate(
                [ratio_re - sums[0] * inverses[i], ratio_im - sums[1] * inverses[i]], axis=1
            )
            high_rows[m], low_rows[m] = parted(cleaned)
    high = jnp.concatenate(high_rows, axis=0)
    low = jnp.concatenate(low_rows, axis=0)
    folded = dot(high, third_ref[0]) + dot(low, third_ref[0]) + dot(high, third_ref[1])

    twirl_cos, twirl_sin = twirl_ref[0], twirl_ref[1]
    columns = []
    for m in range(MS):
        rows = slice(RADIX * m, RADIX * (m + 1))
        re, im = folded[rows, :LANES], folded[rows, LANES:]
        value = jnp.concatenate(
            [re * twirl_cos - im * twirl_sin, re * twirl_sin + im * twirl_cos], axis=0
        )
        high, low = parted(value)
        columns.append(jnp.concatenate([high, high, low], axis=0))
    profile = dot(fourth_ref[...], jnp.concatenate(columns, axis=1))

    pairs = []
    for m in range(MS):
        re = profile[0:8, LANES * m : LANES * (m + 1)]
        im = profile[8:16, LANES * m : LANES * (m + 1)]
        pairs.append(
            (
                jnp.where(lane8 < 64, re, pltpu.roll(im, 64, 1)),
                jnp.where(lane8 < 64, pltpu.roll(re, 64, 1), im),
            )
        )
    for half in range(2):
        for channel in range(2):
            some = [pairs[HS * channel + i][half] for i in range(HS)]
            largest = functools.reduce(jnp.maximum, [jnp.abs(value) for value in some])
            largest = jnp.maximum(jnp.max(largest, axis=1, keepdims=True), 1e-30)
            code = jnp.broadcast_to(jnp.ceil(jnp.log2(largest) * 256.0), (8, LANES))
            inverse = 32767.0 * jnp.exp2(code * (-1.0 / 256.0))
            for i in range(HS):
                value = jnp.clip(jnp.round(some[i] * inverse), -32767.0, 32767.0)
                stage_ref[half, pl.ds(4 * channel + i, 8, stride=8), :] = value.astype(jnp.int32)
            stage_ref[half, pl.ds(4 * channel + HS, 8, stride=8), :] = code.astype(jnp.int32)
        for u in range(8):
            send_ref[2 * u + half] = stage_ref[half, pl.ds(8 * u, 8), :].astype(jnp.int16)

    pl.semaphore_wait(far_sem, 1)
    slot = SUB * sym + 8 * core + pair
    for e, step in EXCHANGE:
        to_sub = stepped(step)
        pltpu.make_async_remote_copy(
            src_ref=send_ref.at[to_sub],
            dst_ref=recv_ref.at[slot],
            send_sem=send_sem,
            recv_sem=recv_sem.at[e],
            device_id={"sym": lax.rem(sym + e, SYM), "sub": to_sub},
            device_id_type=MESH,
        ).start()
    recv_ref[slot] = send_ref[sub]

    cosines = [None] * MS
    sines = [None] * MS
    for e in (0, 1, 3, 2):
        count = SUB - 1 if e == 0 else SUB
        some = recv_ref.at[pl.ds(0, count)]
        pltpu.make_async_remote_copy(
            src_ref=some,
            dst_ref=some,
            send_sem=send_sem,
            recv_sem=recv_sem.at[e],
            device_id={"sub": lax.rem(sub + 1, SUB)},
            device_id_type=MESH,
        ).wait_recv()
        source = lax.rem(sym + SYM - e, SYM)
        base = 8 * SUB * e
        for i in range(SUB):
            got_ref[pl.ds(base + 8 * i, 8), :] = (
                recv_ref[SUB * source + i].astype(jnp.int32).astype(F32)
            )
        for taker in range(2):
            first = base + 64 * taker
            code = got_ref[pl.ds(first + HS, SUB, stride=4), :]
            scale = jnp.exp2(code * (1.0 / 256.0)) * (1.0 / 32767.0)
            for i in range(HS):
                value = got_ref[pl.ds(first + i, SUB, stride=4), :] * scale
                for f in range(MS):
                    at = SYMBOLS * f + MS * source + HS * taker + i
                    c = value * doppler_ref[0, at]
                    n = value * doppler_ref[0, SYMBOLS * MS + at]
                    cosines[f] = c if cosines[f] is None else cosines[f] + c
                    sines[f] = n if sines[f] is None else sines[f] + n
    lane16 = lax.broadcasted_iota(jnp.int32, (SUB, LANES), 1)
    for f in range(MS):
        turned = pltpu.roll(sines[f], 64, 1)
        value = cosines[f] + jnp.where(lane16 < 64, turned, -turned)
        out_ref[0, f, :, :] = value[:, 0:64]
        out_ref[1, f, :, :] = pltpu.roll(value, 64, 1)[:, 0:64]

    index_copies.wait_send()
    for swap in swaps:
        swap.wait_send()
    everything = recv_ref.at[pl.ds(0, SYM * SUB - 1)]
    pltpu.make_async_remote_copy(
        src_ref=everything,
        dst_ref=everything,
        send_sem=send_sem,
        recv_sem=recv_sem.at[0],
        device_id={"sub": lax.rem(sub + 1, SUB)},
        device_id_type=MESH,
    ).wait_send()


def body(samples, constellation_index, pilot_offsets, cp_offset):
    consts = [jnp.asarray(table) for table in tables()]
    vmem = pl.BlockSpec(memory_space=pltpu.VMEM)
    hbm = pl.BlockSpec(memory_space=pl.ANY)
    records = samples.reshape(2 * MS * RECORD, LANES)
    doppler = consts[-1]
    out = pl.pallas_call(
        kernel,
        out_shape=pltpu.VMEM((2, MS, SUB, GUARD // SUB), F32),
        in_specs=[hbm] * (4 + len(consts)),
        out_specs=vmem,
        scratch_shapes=[
            pltpu.SMEM((MS,), jnp.int32),
            pltpu.SMEM((MS,), jnp.int32),
            pltpu.VMEM((4 * HS * RECORD, LANES), F32),
            pltpu.VMEM(constellation_index.shape, jnp.int32),
            *[pltpu.VMEM(table.shape, table.dtype) for table in consts[:-1]],
            pltpu.SMEM((1, doppler.shape[1]), F32),
            pltpu.VMEM((RADIX * MS, 512), BF16),
            pltpu.VMEM((RADIX * MS, 512), BF16),
            pltpu.VMEM((2, 2 * HS, LANES), BF16),
            pltpu.VMEM((SUB, 2 * HS, LANES), BF16),
            pltpu.VMEM((8 * SUB, LANES), F32),
            pltpu.VMEM((2, 64, LANES), jnp.int32),
            pltpu.VMEM((SUB, 8, LANES), jnp.int16),
            pltpu.VMEM((SYM * SUB, 8, LANES), jnp.int16),
            pltpu.VMEM((8 * SYM * SUB, LANES), F32),
            pltpu.SemaphoreType.DMA((14,)),
            pltpu.SemaphoreType.DMA((4,)),
            pltpu.SemaphoreType.DMA,
            pltpu.SemaphoreType.DMA,
            pltpu.SemaphoreType.DMA,
            pltpu.SemaphoreType.DMA((SYM,)),
            pltpu.SemaphoreType.REGULAR,
            pltpu.SemaphoreType.REGULAR,
        ],
        compiler_params=pltpu.CompilerParams(collective_id=0, has_side_effects=True),
    )(cp_offset, pilot_offsets, records, constellation_index, *consts)
    return out.transpose(0, 2, 1, 3)


def solution(mesh):
    return jax.shard_map(
        body,
        mesh=mesh,
        in_specs=(
            P(None, ("chan", "sub"), "sym", None),
            P(("chan", "sym"), "sub"),
            P("sym"),
            P(("chan", "sym")),
        ),
        out_specs=P(None, "chan", "sym", "sub"),
        check_vma=False,
    )
```
